128 devices in a mesh: depth: 4 (over y), track: 32 (over z, x, core).
Axes of the slice: x: 4, y: 4, z: 4, core: 2. Of those that a mesh axis runs over, the one named last changes fastest.
Arguments:
- slowness_cells: float32 [128, 16384], P('depth'), may hold values from 0.5 to 2
- cell_of_group: int32 [512], P('track'), may hold values from 0 to 16383
- taper: float32 [256, 9], replicated, may hold values from 0 to 0.25
- secant: float32 [256], replicated, may hold values from 1 to 3
- primary: bfloat16 [128, 16384, 256], P('depth', 'track'), may hold values from -0.3984375 to 0.3984375
- quadrature: bfloat16 [128, 16384, 256], P('depth', 'track'), may hold values from -0.3984375 to 0.3984375
- observed: float32 [128, 16384], P('depth', 'track'), may hold values from -6 to 6
Outputs:
- focused: float32 [128, 16384], P('depth', 'track')
- gradient: float32 [128, 16384], P('depth')
The draws below stay inside these ranges and needn't reach their ends.
All inputs are finite; a program needn't handle non-finite values.
Results may differ from the reference program's by a relative error of at most 0.0003.
Values sent between devices are 32-bit elements; how exact they have to be, the bound alone decides.
A program may use at most 128 MiB of HBM per device.

```python
import math
import jax
import jax.numpy as jnp
from jax import lax

ANGLES = 256
HALF_WIDTH = 4
NCELL = 16384
Z = 128
X = 16384
GROUPS = 512


def with_ends(values, own_key, low, high):
    extent = values.shape
    place = [jax.random.randint(jax.random.fold_in(own_key, axis), (), 0, extent[axis]) for axis in range(len(extent))]
    values = values.at[tuple(place)].set(low)
    longest = extent.index(max(extent))
    place[longest] = (place[longest] + 1) % extent[longest]
    return values.at[tuple(place)].set(high)


def block_scale(stream_key, extent, cuts, smallest, largest):
    def one(position, shards_of):
        draws = jax.random.uniform(jax.random.fold_in(jax.random.fold_in(stream_key, 6), position), (shards_of,), jnp.float32, smallest / len(cuts), largest / len(cuts))
        return jnp.repeat(jnp.exp(draws), extent[position] // shards_of).reshape((-1,) + (1,) * (len(extent) - position - 1))

    factor_of = one(*cuts[0])
    for cut in cuts[1:]:
        factor_of = factor_of * one(*cut)
    return factor_of


def gaussian(own_key, shape, scale, most, cuts=(), kind=jnp.bfloat16):
    loudness = block_scale(own_key, shape, cuts, -0.22, 0.18) if cuts else 1.0
    values = jax.random.normal(own_key, shape, jnp.float32) * scale * loudness
    return jnp.minimum(jnp.maximum(values, -most), most).astype(kind)


def setup_inputs(seed: int = 0) -> dict:
    streams_of = jax.random.split(jax.random.key(seed), 8)
    return {
        "slowness_cells": jnp.clip(jnp.exp(math.log(2.0) - 1.3862944 * jax.random.uniform(streams_of[0], (Z, NCELL), jnp.float32) ** block_scale(streams_of[0], (Z, NCELL), ((0, 4),), -0.2, 0.2)), 0.5, 2.0),
        "cell_of_group": with_ends(jax.random.randint(streams_of[1], (GROUPS,), 0, NCELL), jax.random.fold_in(streams_of[1], 1), 0, NCELL - 1).astype(jnp.int32),
        "taper": jnp.clip(jax.random.uniform(streams_of[2], (ANGLES, 2 * HALF_WIDTH + 1), jnp.float32, 0.0, 0.25), 0.0, 0.25),
        "secant": jnp.clip(jnp.exp(jax.random.uniform(streams_of[3], (ANGLES,), jnp.float32, math.log(1.0), math.log(3.0))), 1.0, 3.0),
        "primary": gaussian(streams_of[4], (Z, X, ANGLES), 0.0625, 0.3984375, ((0, 4), (1, 32))),
        "quadrature": gaussian(streams_of[5], (Z, X, ANGLES), 0.0625, 0.3984375, ((0, 4), (1, 32))),
        "observed": gaussian(streams_of[6], (Z, X), 1.0, 6.0, ((0, 4), (1, 32)), jnp.float32),
    }


OMEGA = 0.25


def reference(slowness_cells, cell_of_group, taper, secant, primary, quadrature, observed):
    taps = taper.shape[1]
    reach = (taps - 1) // 2
    traces = primary.shape[1]
    group = traces // cell_of_group.shape[0]
    cells = jnp.repeat(cell_of_group, group).astype(jnp.int32)
    slow = jnp.take(slowness_cells, cells, axis=1)
    padded = jnp.pad(slow, ((0, 0), (reach, reach)))
    high = lax.Precision.HIGHEST

    def forward(carry, items):
        row, prim, quad, seen = items
        window = jnp.stack([row[k:k + traces] for k in range(taps)], 0)
        increment = jnp.einsum('kx,ak->xa', window, taper, precision=high) * secant
        travel = carry + increment
        cosine = jnp.cos(OMEGA * travel)
        sine = jnp.sin(OMEGA * travel)
        prim = prim.astype(jnp.float32)
        quad = quad.astype(jnp.float32)
        image = jnp.sum(prim * cosine + quad * sine, axis=1)
        resid = image - seen
        time_grad = OMEGA * resid[:, None] * (quad * cosine - prim * sine)
        return travel, (image, time_grad)

    start = jnp.zeros((traces, taper.shape[0]), jnp.float32)
    _, (focused, time_grad) = lax.scan(forward, start, (padded, primary, quadrature, observed))

    def backward(carry, tgrad):
        step_grad = carry + tgrad
        spread = jnp.einsum('xa,ak->kx', step_grad * secant, taper, precision=high)
        spread = jnp.pad(spread, ((0, 0), (reach, reach)))
        total = jnp.zeros((traces,), jnp.float32)
        for k in range(taps):
            total = total + spread[k, 2 * reach - k:2 * reach - k + traces]
        return step_grad, total

    _, slow_grad = lax.scan(backward, start, time_grad, reverse=True)
    gradient = jax.ops.segment_sum(slow_grad.T, cells, num_segments=slowness_cells.shape[1]).T
    return focused, gradient
```

```python
import functools
import math

import jax
import jax.numpy as jnp
from jax import lax
from jax.experimental import pallas as pl
from jax.experimental.pallas import tpu as pltpu
from jax.sharding import PartitionSpec as P

OMEGA = 0.25
GROUP = 32
LANES = 128
MESH = pl.DeviceIdType.MESH

SIN = (4.442882919178189, -7.308245695274183, 3.6063544029247794, -0.8461128632742358, 0.10982698821149484)
COS = (1.4142134964903517, -6.978850985165349, 5.739461140914948, -1.8835629076104397, 0.310698190958135)

f32 = jnp.float32
bf16 = jnp.bfloat16


def horner(coefs, u):
    value = coefs[-1] * u + coefs[-2]
    for c in coefs[-3::-1]:
        value = value * u + c
    return value


def cos_sin(turns):
    r = turns - jnp.round(turns)
    u = r * r
    s = r * horner(SIN, u)
    c = horner(COS, u)
    return 1.0 - s * s, s * c


def iota(shape, dim):
    return lax.broadcasted_iota(jnp.int32, shape, dim)


def nt(a, b):
    return lax.dot_general(a, b, (((1,), (1,)), ((), ())), preferred_element_type=f32)


def nn(a, b):
    return lax.dot_general(a, b, (((1,), (0,)), ((), ())), preferred_element_type=f32)


def split3(x):
    high = x.astype(bf16).astype(f32)
    rest = x - high
    mid = rest.astype(bf16).astype(f32)
    return jnp.concatenate([high, mid, rest - mid], axis=0).astype(bf16)


def joined3(y):
    n = y.shape[0] // 3
    return y[:n] + y[n : 2 * n] + y[2 * n :]


def one_hot(mask):
    return jnp.where(mask, 1.0, 0.0).astype(bf16)


def peer_of(k, o, nd, nt_):
    d = lax.axis_index("depth")
    t = lax.axis_index("track")
    return (lax.rem(d + k, nd), lax.rem(t + o + nt_, nt_))


def halo_copies(nd, nt_, src, tile, wide, narrow, send, recv):
    copies = []
    for i, o in enumerate((1, -1)):
        copies.append(
            pltpu.make_async_remote_copy(
                src, wide.at[i], send.at[i], recv.at[i], device_id=peer_of(0, o, nd, nt_), device_id_type=MESH
            )
        )
    for k in range(1, nd):
        for o in (-1, 0, 1):
            i = 3 * (k - 1) + o + 1
            copies.append(
                pltpu.make_async_remote_copy(
                    src.at[pl.ds(tile, 8)],
                    narrow.at[i],
                    send.at[2 + i],
                    recv.at[2 + i],
                    device_id=peer_of(k, o, nd, nt_),
                    device_id_type=MESH,
                )
            )
    return copies


def main_kernel(
    nd,
    ntr,
    nchunk,
    slow_hbm,
    cells,
    taper,
    secant,
    prim_hbm,
    quad_hbm,
    seen,
    packets,
    focused,
    slow,
    prim,
    quad,
    weights,
    spread,
    fint,
    bint,
    fedge,
    blo,
    bhi,
    halo_a,
    wide_a,
    narrow_a,
    halo_b,
    wide_b,
    narrow_b,
    mine,
    slow_sem,
    prim_sem,
    quad_sem,
    send_a,
    recv_a,
    send_b,
    recv_b,
    send_c,
    recv_c,
):
    d = lax.axis_index("depth")
    t = lax.axis_index("track")
    depth, traces, angles = prim.shape
    groups = traces // GROUP
    zc = depth // nchunk

    nblock = slow.shape[0]

    def slow_copy(i):
        lanes = pl.ds(pl.multiple_of(i * LANES, LANES), LANES)
        return pltpu.make_async_copy(slow_hbm.at[:, lanes], slow.at[i], slow_sem)

    @pl.loop(0, nblock)
    def _(i):
        slow_copy(i).start()

    def chunk_copies(i):
        rows = pl.ds(i * zc, zc)
        return (
            pltpu.make_async_copy(prim_hbm.at[rows], prim.at[rows], prim_sem.at[i]),
            pltpu.make_async_copy(quad_hbm.at[rows], quad.at[rows], quad_sem.at[i]),
        )

    @pl.loop(0, nchunk)
    def _(i):
        for copy in chunk_copies(i):
            copy.start()

    barrier = pltpu.get_barrier_semaphore()

    @pl.loop(1, ntr)
    def _(k):
        pl.semaphore_signal(barrier, inc=1, device_id=(d, lax.rem(t + k, ntr)), device_id_type=MESH)

    for k in range(1, nd):
        for o in (-1, 0, 1):
            pl.semaphore_signal(barrier, inc=1, device_id=peer_of(k, o, nd, ntr), device_id_type=MESH)

    taps = taper[...].T
    sec = secant[...] * OMEGA
    row = iota((8, angles), 0)
    nlo = jnp.where(row < 4, 4 - row, 12 - row)
    wlo = jnp.zeros((8, angles), f32)
    whi = jnp.zeros((8, angles), f32)
    for k in range(taper.shape[1]):
        tap = jnp.broadcast_to(taps[k : k + 1, :] * sec, (8, angles))
        wlo = wlo + jnp.where(k < nlo, tap, 0.0)
        whi = whi + jnp.where(k < nlo, 0.0, tap)
    weights[0] = wlo
    weights[1] = whi
    weights[2] = jnp.broadcast_to(jnp.sum(taps, axis=0, keepdims=True) * sec, (8, angles))

    nedge = groups * 8
    lane = iota((1, LANES), 1)

    e = iota((nedge, traces), 0)
    x = iota((nedge, traces), 1)
    i = lax.rem(e, 8)
    at = lax.rem((e // 8) * GROUP + jnp.where(i < 4, i, i - 8) + traces, traces)
    edge_of = one_hot(at == x)
    seen_edge = joined3(nt(split3(seen[...]), edge_of))

    @pl.loop(0, nblock)
    def _(i):
        slow_copy(i).wait()

    mine_lane = iota((depth, LANES), 1)
    own = jnp.zeros((depth, LANES), f32)
    for g in range(groups):
        c = cells[g]
        block = slow[lax.div(c, LANES)]
        column = jnp.sum(jnp.where(mine_lane == lax.rem(c, LANES), block, 0.0), axis=1, keepdims=True)
        own = jnp.where(mine_lane == g, column, own)
    zrow = iota((depth, LANES), 0)
    s = 1
    while s < depth:
        own = own + jnp.where(zrow >= s, pltpu.roll(own, s, 0), 0.0)
        s *= 2
    halo_a[...] = own

    pl.semaphore_wait(barrier, ntr - 1 + 3 * (nd - 1))
    copies = halo_copies(nd, ntr, halo_a, depth - 8, wide_a, narrow_a, send_a, recv_a)
    for copy in copies:
        copy.start()
    for copy in copies:
        copy.wait()

    def total(o, rowi, narrow, up):
        acc = jnp.zeros((1, LANES), f32)
        for k in range(1, nd):
            use = (k <= d) if up else (k > d)
            acc = acc + jnp.where(use, narrow[3 * (k - 1) + o + 1, rowi : rowi + 1, :], 0.0)
        return acc

    centre = own + total(0, 7, narrow_a, True)
    left = jnp.where(t > 0, wide_a[0] + total(1, 7, narrow_a, True), 0.0)
    right = jnp.where(t < ntr - 1, wide_a[1] + total(-1, 7, narrow_a, True), 0.0)
    summed = jnp.where(mine_lane < groups, centre, 0.0)
    summed = jnp.where(mine_lane == groups, pltpu.roll(left, 1, 1), summed)
    summed = jnp.where(mine_lane == groups + 1, pltpu.roll(right, groups + 1, 1), summed)
    halo_a[...] = summed * (1.0 / (2.0 * math.pi))

    nrow = spread.shape[1]
    diagonal = iota((nrow, LANES), 0) == iota((nrow, LANES), 1)

    @pl.loop(0, depth, unroll=4)
    def _(z):
        line = jnp.broadcast_to(halo_a[pl.ds(z, 1), :], (nrow, LANES))
        spread[z] = jnp.broadcast_to(
            jnp.sum(jnp.where(diagonal, line, 0.0), axis=1, keepdims=True), (nrow, LANES)
        )

    sub = iota((8, angles), 0)
    upper = sub < 4
    sub128 = iota((8, LANES), 0)
    lane128 = iota((8, LANES), 1)
    place = lax.rem(lane128, 8) == sub128
    half = 256
    own_group = sub == iota((8, half), 1) // GROUP

    def each_depth(z):
        for h in range(traces // half):
            first = h * half // GROUP
            c8 = spread[z, first : first + 8, :]
            w = weights[2]
            c, s = cos_sin(w * jnp.concatenate([c8] * (angles // LANES), axis=1))
            wc = w * c
            ws = w * s

            def pair(v):
                return [v, v - v.astype(bf16).astype(f32)]

            lhs_p = jnp.concatenate(pair(c) + pair(-ws), axis=0).astype(bf16)
            lhs_q = jnp.concatenate(pair(s) + pair(wc), axis=0).astype(bf16)
            rows = pl.ds(h * half, half)
            out = nt(lhs_p, prim[z, rows, :]) + nt(lhs_q, quad[z, rows, :])
            fsum = jnp.where(own_group, out[0:8] + out[8:16], 0.0)
            bsum = jnp.where(own_group, out[16:24] + out[24:32], 0.0)
            fint[pl.ds(z, 1), rows] = jnp.sum(fsum, axis=0, keepdims=True)
            bint[pl.ds(z, 1), rows] = jnp.sum(bsum, axis=0, keepdims=True)
        acc_f = jnp.zeros((8, LANES), f32)
        acc_lo = jnp.zeros((8, LANES), f32)
        acc_hi = jnp.zeros((8, LANES), f32)
        for b in range(groups):

            def splat(r):
                return jnp.broadcast_to(spread[z, r : r + 1, :], (8, LANES))

            if b == 0:
                clo = jnp.where(sub128 < 4, splat(groups), splat(groups - 1))
                chi = jnp.where(sub128 < 4, splat(0), splat(groups + 1))
            else:
                clo = splat(b - 1)
                chi = splat(b)
            clo = jnp.concatenate([clo] * (angles // LANES), axis=1)
            chi = jnp.concatenate([chi] * (angles // LANES), axis=1)

            def edge_rows(ref):
                behind = ref[z, GROUP * b : GROUP * b + 8, :].astype(f32)
                stop = GROUP * b if b else traces
                before = ref[z, stop - 8 : stop, :].astype(f32)
                return jnp.where(upper, behind, before)

            pe = edge_rows(prim)
            qe = edge_rows(quad)
            wlo = weights[0]
            whi = weights[1]
            c, s = cos_sin(wlo * clo + whi * chi)
            g = qe * c - pe * s
            here = lane128 // 8 == b
            acc_f = jnp.where(here, jnp.sum(pe * c + qe * s, axis=1, keepdims=True), acc_f)
            acc_lo = jnp.where(here, jnp.sum(g * wlo, axis=1, keepdims=True), acc_lo)
            acc_hi = jnp.where(here, jnp.sum(g * whi, axis=1, keepdims=True), acc_hi)
        for acc, ref in ((acc_f, fedge), (acc_lo, blo), (acc_hi, bhi)):
            ref[pl.ds(z, 1), :] = jnp.sum(jnp.where(place, acc, 0.0), axis=0, keepdims=True)

    @pl.loop(0, nchunk)
    def _(i):
        for copy in chunk_copies(i):
            copy.wait()

        @pl.loop(0, zc)
        def _(j):
            each_depth(i * zc + j)

    xoff = lax.rem(iota((depth, traces), 1), GROUP)
    inner = (xoff >= 4) & (xoff < GROUP - 4)
    term = jnp.where(inner, (fint[...] - seen[...]) * bint[...], 0.0)
    resid = fedge[...] - seen_edge
    xg = iota((traces, LANES), 0) // GROUP
    to_own = one_hot(xg == iota((traces, LANES), 1))
    eb = iota((nedge, LANES), 0)
    el = iota((nedge, LANES), 1)
    bi = eb // 8
    upper_row = lax.rem(eb, 8) < 4
    lo_target = jnp.where(bi > 0, bi - 1, jnp.where(upper_row, groups, groups - 1))
    hi_target = jnp.where((bi > 0) | upper_row, bi, groups + 1)
    sums = joined3(nn(split3(term), to_own))
    sums = sums + joined3(nn(split3(resid * blo[...]), one_hot(lo_target == el)))
    sums = sums + joined3(nn(split3(resid * bhi[...]), one_hot(hi_target == el)))
    s = 1
    while s < depth:
        sums = sums + jnp.where(zrow < depth - s, pltpu.roll(sums, depth - s, 0), 0.0)
        s *= 2
    halo_b[...] = sums

    copies = halo_copies(nd, ntr, halo_b, 0, wide_b, narrow_b, send_b, recv_b)
    for copy in copies:
        copy.start()
    full = jnp.where(inner, fint[...], joined3(nn(split3(fedge[...]), edge_of)))
    focused[...] = full
    cell_lanes = jnp.zeros((8, LANES), f32)
    for g in range(groups):
        cell_lanes = jnp.where(lane128 == 4 * groups + g, cells[g].astype(f32), cell_lanes)
    for copy in copies:
        copy.wait()

    centre = sums + total(0, 0, narrow_b, False)
    left = jnp.where(t > 0, wide_b[0] + total(1, 0, narrow_b, False), 0.0)
    right = jnp.where(t < ntr - 1, wide_b[1] + total(-1, 0, narrow_b, False), 0.0)
    grads = jnp.where(mine_lane < groups, centre, 0.0)
    grads = grads + jnp.where(mine_lane == 0, pltpu.roll(left, LANES - groups - 1, 1), 0.0)
    grads = grads + jnp.where(mine_lane == groups - 1, pltpu.roll(right, LANES - 1, 1), 0.0)
    packet = cell_lanes
    for q in range(depth // 8):
        block = grads[8 * q : 8 * q + 8]
        packet = packet + (pltpu.roll(block, groups * q, 1) if q else block)
    per = LANES // groups
    packet = pltpu.roll(packet, groups * lax.rem(t, per), 1)
    mine[...] = packet
    packets[t] = packet

    def packet_copy(k):
        return pltpu.make_async_remote_copy(
            mine,
            packets.at[t],
            send_c.at[k],
            recv_c.at[k],
            device_id=(d, lax.rem(t + k, ntr)),
            device_id_type=MESH,
        )

    def packet_arrival(k):
        return pltpu.make_async_remote_copy(
            mine,
            packets.at[lax.rem(t + ntr - k, ntr)],
            send_c.at[k],
            recv_c.at[k],
            device_id=(d, lax.rem(t + k, ntr)),
            device_id_type=MESH,
        )

    @pl.loop(1, ntr)
    def _(k):
        packet_copy(k).start()

    @pl.loop(1, ntr)
    def _(k):
        packet_copy(k).wait_send()
        packet_arrival(k).wait_recv()


WIDE = 256
STEPS = 8


def scatter_kernel(groups, packets, focused, grad, image, ghigh, glow, block_of, place):
    ntr = packets.shape[0]
    per = LANES // groups
    depth = grad.shape[0]
    total = ntr * groups
    step = pl.program_id(0)

    @pl.when(step == 0)
    def _():
        image[...] = focused[...]
        chunk = iota((8, LANES), 1) // groups
        for col in range(ntr // per):
            parts = []
            for q in range(depth // 8 + 1):
                acc = jnp.zeros((8, LANES), f32)
                for j in range(per):
                    acc = jnp.where(chunk == (q + j) % per, packets[col * per + j], acc)
                parts.append(pltpu.roll(acc, LANES - groups * q, 1) if q else acc)
            at = pl.ds(col * LANES, LANES)
            g = jnp.concatenate(parts[:-1], axis=0)
            high = g.astype(bf16)
            ghigh[:, at] = high
            glow[:, at] = (g - high.astype(f32)).astype(bf16)
            cell = parts[-1][0:1]
            block = jnp.floor(cell * (1.0 / WIDE))
            block_of[:, at] = jnp.broadcast_to(block, (depth, LANES)).astype(bf16)
            inside = cell - block * WIDE
            place[:, at] = one_hot(iota((WIDE, LANES), 0).astype(f32) == inside)

    nblock = grad.shape[1] // WIDE
    highs = []
    lows = []
    for j in range(nblock):
        mask = block_of[...] == (step * nblock + j).astype(bf16)
        highs.append(jnp.where(mask, ghigh[...], jnp.zeros((), bf16)))
        lows.append(jnp.where(mask, glow[...], jnp.zeros((), bf16)))
    out = nt(jnp.concatenate(highs, axis=0), place[...]) + nt(jnp.concatenate(lows, axis=0), place[...])
    for j in range(nblock):
        grad[:, j * WIDE : (j + 1) * WIDE] = out[depth * j : depth * (j + 1)]


def on_device(nd, ntr, slowness_cells, cell_of_group, taper, secant, primary, quadrature, observed):
    depth, traces, angles = primary.shape
    ncell = slowness_cells.shape[1]
    groups = cell_of_group.shape[0]
    nchunk = 8
    vmem = pl.BlockSpec(memory_space=pltpu.VMEM)
    anywhere = pl.BlockSpec(memory_space=pltpu.HBM)
    nhalo = 2 + 3 * (nd - 1)
    dma = pltpu.SemaphoreType.DMA
    packets, focused = pl.pallas_call(
        functools.partial(main_kernel, nd, ntr, nchunk),
        out_shape=(
            jax.ShapeDtypeStruct((ntr, 8, LANES), f32),
            jax.ShapeDtypeStruct((depth, traces), f32),
        ),
        in_specs=[anywhere, pl.BlockSpec(memory_space=pltpu.SMEM), vmem, vmem, anywhere, anywhere, vmem],
        out_specs=(vmem, vmem),
        scratch_shapes=[
            pltpu.VMEM((ncell // LANES, depth, LANES), f32),
            pltpu.VMEM((depth, traces, angles), bf16),
            pltpu.VMEM((depth, traces, angles), bf16),
            pltpu.VMEM((3, 8, angles), f32),
            pltpu.VMEM((depth, 24, LANES), f32),
            pltpu.VMEM((depth, traces), f32),
            pltpu.VMEM((depth, traces), f32),
            pltpu.VMEM((depth, LANES), f32),
            pltpu.VMEM((depth, LANES), f32),
            pltpu.VMEM((depth, LANES), f32),
            pltpu.VMEM((depth, LANES), f32),
            pltpu.VMEM((2, depth, LANES), f32),
            pltpu.VMEM((3 * (nd - 1), 8, LANES), f32),
            pltpu.VMEM((depth, LANES), f32),
            pltpu.VMEM((2, depth, LANES), f32),
            pltpu.VMEM((3 * (nd - 1), 8, LANES), f32),
            pltpu.VMEM((8, LANES), f32),
            dma,
            dma((nchunk,)),
            dma((nchunk,)),
            dma((nhalo,)),
            dma((nhalo,)),
            dma((nhalo,)),
            dma((nhalo,)),
            dma((ntr,)),
            dma((ntr,)),
        ],
        compiler_params=pltpu.CompilerParams(
            collective_id=0, has_side_effects=True, vmem_limit_bytes=63 * 1024 * 1024
        ),
        name="radargram",
    )(slowness_cells, cell_of_group, taper, secant.reshape(1, angles), primary, quadrature, observed)

    wide = ncell // STEPS
    gradient, image = pl.pallas_call(
        functools.partial(scatter_kernel, groups),
        out_shape=(
            jax.ShapeDtypeStruct((depth, ncell), f32),
            jax.ShapeDtypeStruct((depth, traces), f32),
        ),
        grid=(STEPS,),
        in_specs=[
            pl.BlockSpec((ntr, 8, LANES), lambda i: (0, 0, 0)),
            pl.BlockSpec((depth, traces), lambda i: (0, 0)),
        ],
        out_specs=(
            pl.BlockSpec((depth, wide), lambda i: (0, i)),
            pl.BlockSpec((depth, traces), lambda i: (0, 0)),
        ),
        scratch_shapes=[
            pltpu.VMEM((depth, ntr * groups), bf16),
            pltpu.VMEM((depth, ntr * groups), bf16),
            pltpu.VMEM((depth, ntr * groups), bf16),
            pltpu.VMEM((WIDE, ntr * groups), bf16),
        ],
        compiler_params=pltpu.CompilerParams(dimension_semantics=("arbitrary",)),
        name="scatter",
    )(packets, focused)
    return image, gradient


def solution(mesh):
    in_specs = (
        P("depth", None),
        P("track"),
        P(),
        P(),
        P("depth", "track", None),
        P("depth", "track", None),
        P("depth", "track"),
    )
    out_specs = (P("depth", "track"), P("depth", None))
    nd = mesh.shape["depth"]
    ntr = mesh.shape["track"]
    return jax.shard_map(
        functools.partial(on_device, nd, ntr), mesh=mesh, in_specs=in_specs, out_specs=out_specs, check_vma=False
    )
```

```python
import functools
import math

import jax
import jax.numpy as jnp
from jax import lax
from jax.experimental import pallas as pl
from jax.experimental.pallas import tpu as pltpu
from jax.sharding import PartitionSpec as P

OMEGA = 0.25
GROUP = 32
LANES = 128
MESH = pl.DeviceIdType.MESH

SIN = (4.442882919178189, -7.308245695274183, 3.6063544029247794, -0.8461128632742358, 0.10982698821149484)
COS = (1.4142134964903517, -6.978850985165349, 5.739461140914948, -1.8835629076104397, 0.310698190958135)

f32 = jnp.float32
bf16 = jnp.bfloat16


def horner(coefs, u):
    value = coefs[-1] * u + coefs[-2]
    for c in coefs[-3::-1]:
        value = value * u + c
    return value


def cos_sin(turns):
    r = turns - jnp.round(turns)
    u = r * r
    s = r * horner(SIN, u)
    c = horner(COS, u)
    return 1.0 - s * s, s * c


def iota(shape, dim):
    return lax.broadcasted_iota(jnp.int32, shape, dim)


def nt(a, b):
    return lax.dot_general(a, b, (((1,), (1,)), ((), ())), preferred_element_type=f32)


def nn(a, b):
    return lax.dot_general(a, b, (((1,), (0,)), ((), ())), preferred_element_type=f32)


def split3(x):
    high = x.astype(bf16).astype(f32)
    rest = x - high
    mid = rest.astype(bf16).astype(f32)
    return jnp.concatenate([high, mid, rest - mid], axis=0).astype(bf16)


def joined3(y):
    n = y.shape[0] // 3
    return y[:n] + y[n : 2 * n] + y[2 * n :]


def one_hot(mask):
    return jnp.where(mask, 1.0, 0.0).astype(bf16)


def peer_of(k, o, nd, nt_):
    d = lax.axis_index("depth")
    t = lax.axis_index("track")
    return (lax.rem(d + k, nd), lax.rem(t + o + nt_, nt_))


def near_copies(nd, nt_, src, tile, into, send, recv):
    return [
        pltpu.make_async_remote_copy(
            src.at[pl.ds(tile, 8)],
            into.at[k - 1],
            send.at[k - 1],
            recv.at[k - 1],
            device_id=peer_of(k, 0, nd, nt_),
            device_id_type=MESH,
        )
        for k in range(1, nd)
    ]


def side_copies(nd, nt_, src, tile, wide, narrow, send, recv):
    copies = []
    for i, o in enumerate((1, -1)):
        copies.append(
            pltpu.make_async_remote_copy(
                src, wide.at[i], send.at[i], recv.at[i], device_id=peer_of(0, o, nd, nt_), device_id_type=MESH
            )
        )
    for k in range(1, nd):
        for i, o in enumerate((1, -1)):
            at = 2 * (k - 1) + i
            copies.append(
                pltpu.make_async_remote_copy(
                    src.at[pl.ds(tile, 8)],
                    narrow.at[at],
                    send.at[2 + at],
                    recv.at[2 + at],
                    device_id=peer_of(k, o, nd, nt_),
                    device_id_type=MESH,
                )
            )
    return copies


WIDE = 256
PER_STEP = 8


def main_kernel(
    nd,
    ntr,
    nchunk,
    slow_hbm,
    cells_hbm,
    taper_hbm,
    secant_hbm,
    prim_hbm,
    quad_hbm,
    seen_hbm,
    grad,
    focused,
    cells,
    taper,
    secant,
    seen,
    slow,
    prim,
    quad,
    weights,
    line,
    spread,
    fint,
    bint,
    fedge,
    blo,
    bhi,
    fside,
    loside,
    hiside,
    edge_of,
    to_own,
    to_lo,
    to_hi,
    halo_a,
    near_a,
    wide_a,
    narrow_a,
    halo_b,
    wide_b,
    narrow_b,
    halo_c,
    near_c,
    mine,
    packets,
    below_mine,
    belows,
    ghigh,
    glow,
    block_of,
    place_of,
    rows_of,
    small_sem,
    slow_sem,
    prim_sem,
    quad_sem,
    send_a,
    recv_a,
    send_as,
    recv_as,
    send_b,
    recv_b,
    send_c,
    recv_c,
    send_p,
    recv_p,
    send_q,
    recv_q,
):
    d = lax.axis_index("depth")
    t = lax.axis_index("track")
    depth, traces, angles = prim.shape
    groups = traces // GROUP
    zc = depth // nchunk
    per = LANES // groups

    barrier = pltpu.get_barrier_semaphore()
    slow_copy = pltpu.make_async_copy(slow_hbm, slow, slow_sem)
    small = [
        pltpu.make_async_copy(cells_hbm, cells, small_sem.at[0]),
        pltpu.make_async_copy(taper_hbm, taper, small_sem.at[1]),
        pltpu.make_async_copy(secant_hbm, secant, small_sem.at[2]),
        pltpu.make_async_copy(seen_hbm, seen, small_sem.at[3]),
    ]
    small[0].start()
    slow_copy.start()

    @pl.loop(1, ntr)
    def _(k):
        pl.semaphore_signal(barrier, inc=1, device_id=(d, lax.rem(t + k, ntr)), device_id_type=MESH)

    for k in range(1, nd):
        for o in (-1, 0, 1):
            pl.semaphore_signal(barrier, inc=1, device_id=peer_of(k, o, nd, ntr), device_id_type=MESH)
    for copy in small[1:]:
        copy.start()

    def chunk_copies(i):
        rows = pl.ds(i * zc, zc)
        return (
            pltpu.make_async_copy(prim_hbm.at[rows], prim.at[rows], prim_sem.at[i]),
            pltpu.make_async_copy(quad_hbm.at[rows], quad.at[rows], quad_sem.at[i]),
        )

    mine_lane = iota((depth, LANES), 1)
    zrow = iota((depth, LANES), 0)
    small[0].wait()
    slow_copy.wait()

    @pl.loop(0, nchunk)
    def _(i):
        for copy in chunk_copies(i):
            copy.start()

    own = jnp.zeros((depth, LANES), f32)
    for g in range(groups):
        c = cells[g]
        block = slow[:, lax.div(c, LANES)].reshape(depth, LANES)
        column = jnp.sum(jnp.where(mine_lane == lax.rem(c, LANES), block, 0.0), axis=1, keepdims=True)
        own = jnp.where(mine_lane == g, column, own)
    s = 1
    while s < depth:
        own = own + jnp.where(zrow >= s, pltpu.roll(own, s, 0), 0.0)
        s *= 2
    halo_a[...] = own

    pl.semaphore_wait(barrier, ntr - 1 + 3 * (nd - 1))
    near = near_copies(nd, ntr, halo_a, depth - 8, near_a, send_a, recv_a)
    side_a = side_copies(nd, ntr, halo_a, depth - 8, wide_a, narrow_a, send_as, recv_as)
    for copy in near + side_a:
        copy.start()

    for copy in small[1:]:
        copy.wait()
    taps = taper[...]
    sec = secant[...] * OMEGA
    row = iota((8, angles), 0)
    nlo = jnp.where(row < 4, 4 - row, 12 - row)
    wlo = jnp.zeros((8, angles), f32)
    whi = jnp.zeros((8, angles), f32)
    for k in range(taper.shape[0]):
        tap = jnp.broadcast_to(taps[k : k + 1, :] * sec, (8, angles))
        wlo = wlo + jnp.where(k < nlo, tap, 0.0)
        whi = whi + jnp.where(k < nlo, 0.0, tap)
    weights[0] = wlo
    weights[1] = whi
    weights[2] = jnp.broadcast_to(jnp.sum(taps, axis=0, keepdims=True) * sec, (8, angles))

    nedge = groups * 8
    e = iota((nedge, traces), 0)
    x = iota((nedge, traces), 1)
    i = lax.rem(e, 8)
    at = lax.rem(lax.div(e, 8) * GROUP + jnp.where(i < 4, i, i - 8) + traces, traces)
    edge_of[...] = one_hot(at == x)
    to_own[...] = one_hot(lax.div(iota((traces, LANES), 0), GROUP) == iota((traces, LANES), 1))
    eb = iota((nedge, LANES), 0)
    el = iota((nedge, LANES), 1)
    bi = lax.div(eb, 8)
    behind_row = lax.rem(eb, 8) < 4
    to_lo[...] = one_hot(jnp.where(bi > 0, bi - 1, jnp.where(behind_row, groups, groups - 1)) == el)
    to_hi[...] = one_hot(jnp.where((bi > 0) | behind_row, bi, groups + 1) == el)
    seen_edge = joined3(nt(split3(seen[...]), edge_of[...]))

    for copy in near:
        copy.wait()

    def near_total(into, rowi, up):
        acc = jnp.zeros((1, LANES), f32)
        for k in range(1, nd):
            acc = acc + jnp.where((k <= d) if up else (k > d), into[k - 1, rowi : rowi + 1, :], 0.0)
        return acc

    def side_total(i, rowi, narrow, up):
        acc = jnp.zeros((1, LANES), f32)
        for k in range(1, nd):
            use = (k <= d) if up else (k > d)
            acc = acc + jnp.where(use, narrow[2 * (k - 1) + i, rowi : rowi + 1, :], 0.0)
        return acc

    turn = 1.0 / (2.0 * math.pi)
    line[...] = (own + near_total(near_a, 7, True)) * turn

    def spread_rows(first, count):
        diagonal = iota((count, LANES), 0) + first == iota((count, LANES), 1)

        @pl.loop(0, depth, unroll=8)
        def _(z):
            lines = jnp.broadcast_to(line[pl.ds(z, 1), :], (count, LANES))
            spread[z, first : first + count, :] = jnp.broadcast_to(
                jnp.sum(jnp.where(diagonal, lines, 0.0), axis=1, keepdims=True), (count, LANES)
            )

    spread_rows(0, groups)

    sub = iota((8, angles), 0)
    upper = sub < 4
    sub128 = iota((8, LANES), 0)
    lane128 = iota((8, LANES), 1)
    place = lax.rem(lane128, 8) == sub128
    half = 256
    own_group = sub == lax.div(iota((8, half), 1), GROUP)

    def splat(z, r):
        return jnp.broadcast_to(spread[z, r : r + 1, :], (8, LANES))

    def edge_sums(z, b, clo, chi):
        clo = jnp.concatenate([clo] * (angles // LANES), axis=1)
        chi = jnp.concatenate([chi] * (angles // LANES), axis=1)

        def edge_rows(ref):
            behind = ref[z, GROUP * b : GROUP * b + 8, :].astype(f32)
            stop = GROUP * b if b else traces
            before = ref[z, stop - 8 : stop, :].astype(f32)
            return jnp.where(upper, behind, before)

        pe = edge_rows(prim)
        qe = edge_rows(quad)
        wlo = weights[0]
        whi = weights[1]
        c, s = cos_sin(wlo * clo + whi * chi)
        g = qe * c - pe * s
        return [jnp.sum(v, axis=1, keepdims=True) for v in (pe * c + qe * s, g * wlo, g * whi)]

    def each_depth(z):
        for h in range(traces // half):
            first = h * half // GROUP
            c8 = spread[z, first : first + 8, :]
            w = weights[2]
            c, s = cos_sin(w * jnp.concatenate([c8] * (angles // LANES), axis=1))
            wc = w * c
            ws = w * s

            def pair(v):
                return [v, v - v.astype(bf16).astype(f32)]

            lhs_p = jnp.concatenate(pair(c) + pair(-ws), axis=0).astype(bf16)
            lhs_q = jnp.concatenate(pair(s) + pair(wc), axis=0).astype(bf16)
            rows = pl.ds(h * half, half)
            out = nt(lhs_p, prim[z, rows, :]) + nt(lhs_q, quad[z, rows, :])
            fsum = jnp.where(own_group, out[0:8] + out[8:16], 0.0)
            bsum = jnp.where(own_group, out[16:24] + out[24:32], 0.0)
            fint[pl.ds(z, 1), rows] = jnp.sum(fsum, axis=0, keepdims=True)
            bint[pl.ds(z, 1), rows] = jnp.sum(bsum, axis=0, keepdims=True)
        accs = [jnp.zeros((8, LANES), f32)] * 3
        for b in range(1, groups):
            here = lax.div(lane128, 8) == b
            found = edge_sums(z, b, splat(z, b - 1), splat(z, b))
            accs = [jnp.where(here, v, acc) for v, acc in zip(found, accs)]
        for acc, ref in zip(accs, (fedge, blo, bhi)):
            ref[pl.ds(z, 1), :] = jnp.sum(jnp.where(place, acc, 0.0), axis=0, keepdims=True)

    def outer_edge(z):
        clo = jnp.where(sub128 < 4, splat(z, groups), splat(z, groups - 1))
        chi = jnp.where(sub128 < 4, splat(z, 0), splat(z, groups + 1))
        found = edge_sums(z, 0, clo, chi)
        for v, ref in zip(found, (fside, loside, hiside)):
            picked = jnp.where(place & (lane128 < 8), v, 0.0)
            ref[pl.ds(z, 1), :] = jnp.sum(picked, axis=0, keepdims=True)

    @pl.loop(0, nchunk // 2)
    def _(i):
        for copy in chunk_copies(i):
            copy.wait()

        @pl.loop(0, zc, unroll=UNROLL)
        def _(j):
            each_depth(i * zc + j)

    for i in range(nchunk // 2, nchunk):
        for copy in chunk_copies(i):
            copy.wait()

    for copy in side_a:
        copy.wait()
    left = jnp.where(t > 0, wide_a[0] + side_total(0, 7, narrow_a, True), 0.0) * turn
    right = jnp.where(t < ntr - 1, wide_a[1] + side_total(1, 7, narrow_a, True), 0.0) * turn
    outer = jnp.where(mine_lane == groups, pltpu.roll(left, 1, 1), 0.0)
    line[...] = jnp.where(mine_lane == groups + 1, pltpu.roll(right, groups + 1, 1), outer)
    spread_rows(groups, 8)

    @pl.loop(0, depth, unroll=8)
    def _(z):
        outer_edge(z)

    def suffix(v):
        s = 1
        while s < depth:
            v = v + jnp.where(zrow < depth - s, pltpu.roll(v, depth - s, 0), 0.0)
            s *= 2
        return v

    resid = fside[...] - seen_edge
    to_left = jnp.sum(jnp.where(mine_lane < 4, resid * loside[...], 0.0), axis=1, keepdims=True)
    to_right = jnp.sum(
        jnp.where((mine_lane >= 4) & (mine_lane < 8), resid * hiside[...], 0.0), axis=1, keepdims=True
    )
    halo_b[...] = suffix(
        jnp.where(mine_lane == groups, to_left, jnp.where(mine_lane == groups + 1, to_right, 0.0))
    )
    side_b = side_copies(nd, ntr, halo_b, 0, wide_b, narrow_b, send_b, recv_b)
    for copy in side_b:
        copy.start()

    @pl.loop(depth // 2, depth, unroll=UNROLL)
    def _(z):
        each_depth(z)

    xoff = lax.rem(iota((depth, traces), 1), GROUP)
    inner = (xoff >= 4) & (xoff < GROUP - 4)
    term = jnp.where(inner, (fint[...] - seen[...]) * bint[...], 0.0)
    edge = fedge[...] + fside[...]
    resid = edge - seen_edge
    sums = joined3(nn(split3(term), to_own[...]))
    sums = sums + joined3(nn(split3(resid * (blo[...] + loside[...])), to_lo[...]))
    sums = sums + joined3(nn(split3(resid * (bhi[...] + hiside[...])), to_hi[...]))
    sums = suffix(sums)
    halo_c[...] = sums
    near = near_copies(nd, ntr, halo_c, 0, near_c, send_c, recv_c)
    for copy in near:
        copy.start()

    for copy in side_b:
        copy.wait()
    left = jnp.where(t > 0, wide_b[0] + side_total(0, 0, narrow_b, False), 0.0)
    right = jnp.where(t < ntr - 1, wide_b[1] + side_total(1, 0, narrow_b, False), 0.0)
    grads = jnp.where(mine_lane < groups, sums, 0.0)
    grads = grads + jnp.where(mine_lane == 0, pltpu.roll(left, LANES - groups - 1, 1), 0.0)
    grads = grads + jnp.where(mine_lane == groups - 1, pltpu.roll(right, LANES - 1, 1), 0.0)
    packet = jnp.zeros((8, LANES), f32)
    for g in range(groups):
        packet = jnp.where(lane128 == 4 * groups + g, cells[g].astype(f32), packet)
    for q in range(depth // 8):
        block = grads[8 * q : 8 * q + 8]
        packet = packet + (pltpu.roll(block, groups * q, 1) if q else block)
    shift = groups * lax.rem(t, per)
    packet = pltpu.roll(packet, shift, 1)
    mine[...] = packet
    packets[t] = packet

    def track_copy(k, src, into, send, recv, sender):
        return pltpu.make_async_remote_copy(
            src,
            into.at[sender],
            send.at[k],
            recv.at[k],
            device_id=(d, lax.rem(t + k, ntr)),
            device_id_type=MESH,
        )

    def sent(k, src, into, send, recv):
        return track_copy(k, src, into, send, recv, t)

    def arrived(k, src, into, send, recv):
        return track_copy(k, src, into, send, recv, lax.rem(t + ntr - k, ntr))

    first = (mine, packets, send_p, recv_p)
    second = (below_mine, belows, send_q, recv_q)

    @pl.loop(1, ntr)
    def _(k):
        sent(k, *first).start()

    for copy in near:
        copy.wait()
    below = jnp.where(lane128 < groups, jnp.broadcast_to(near_total(near_c, 0, False), (8, LANES)), 0.0)
    below = pltpu.roll(below, shift, 1)
    below_mine[...] = below
    belows[t] = below

    @pl.loop(1, ntr)
    def _(k):
        sent(k, *second).start()

    focused[...] = jnp.where(inner, fint[...], joined3(nn(split3(edge), edge_of[...])))

    @pl.loop(1, ntr)
    def _(k):
        arrived(k, *first).wait_recv()

    chunk = lax.div(lane128, groups)
    for col in range(ntr // per):
        parts = []
        for q in range(depth // 8 + 1):
            acc = jnp.zeros((8, LANES), f32)
            for j in range(per):
                acc = jnp.where(chunk == (q + j) % per, packets[col * per + j], acc)
            parts.append(pltpu.roll(acc, LANES - groups * q, 1) if q else acc)
        lanes = pl.ds(col * LANES, LANES)
        g = jnp.concatenate(parts[:-1], axis=0)
        high = g.astype(bf16)
        ghigh[:, lanes] = high
        glow[:, lanes] = (g - high.astype(f32)).astype(bf16)
        cell = parts[-1][0:1]
        block = jnp.floor(cell * (1.0 / WIDE))
        block_of[:, lanes] = jnp.broadcast_to(block, (depth, LANES)).astype(bf16)
        place_of[:, lanes] = one_hot(iota((WIDE, LANES), 0).astype(f32) == cell - block * WIDE)

    nblock = grad.shape[1] // WIDE

    @pl.loop(0, nblock // PER_STEP)
    def _(step):
        highs = []
        lows = []
        for j in range(PER_STEP):
            mask = block_of[...] == (step * PER_STEP + j).astype(bf16)
            highs.append(jnp.where(mask, ghigh[...], jnp.zeros((), bf16)))
            lows.append(jnp.where(mask, glow[...], jnp.zeros((), bf16)))
        out = nt(jnp.concatenate(highs, axis=0), place_of[...]) + nt(jnp.concatenate(lows, axis=0), place_of[...])
        out = jnp.concatenate([out[depth * j : depth * (j + 1)] for j in range(PER_STEP)], axis=1)
        wide = PER_STEP * WIDE
        grad[:, pl.ds(pl.multiple_of(step * wide, wide), wide)] = out

    @pl.loop(1, ntr)
    def _(k):
        arrived(k, *second).wait_recv()

    cols = []
    for col in range(ntr // per):
        acc = belows[col * per, 0:1, :]
        for j in range(1, per):
            acc = acc + belows[col * per + j, 0:1, :]
        cols.append(acc)
    below = jnp.broadcast_to(jnp.concatenate(cols, axis=1), (nblock, ntr * groups))
    blocks = jnp.broadcast_to(block_of[...].astype(f32)[0:1], (nblock, ntr * groups))
    spread_below = jnp.where(blocks == iota((nblock, ntr * groups), 0).astype(f32), below, 0.0)
    rows_of[...] = joined3(nt(split3(spread_below), place_of[...]))

    @pl.loop(0, nblock, unroll=8)
    def _(j):
        lanes = pl.ds(pl.multiple_of(j * WIDE, WIDE), WIDE)
        grad[:, lanes] = grad[:, lanes] + jnp.broadcast_to(rows_of[pl.ds(j, 1), :], (depth, WIDE))

    @pl.loop(1, ntr)
    def _(k):
        sent(k, *first).wait_send()
        sent(k, *second).wait_send()


UNROLL = 2


def on_device(nd, ntr, slowness_cells, cell_of_group, taper, secant, primary, quadrature, observed):
    depth, traces, angles = primary.shape
    taps = taper.shape[1]
    ncell = slowness_cells.shape[1]
    groups = cell_of_group.shape[0]
    nedge = groups * 8
    total = ntr * groups
    nchunk = 8
    vmem = pl.BlockSpec(memory_space=pltpu.VMEM)
    anywhere = pl.BlockSpec(memory_space=pl.ANY)
    near = nd - 1
    side = 2 * nd
    dma = pltpu.SemaphoreType.DMA
    V = pltpu.VMEM
    slow = slowness_cells.reshape(depth // 8, 8, ncell // LANES, LANES).transpose(0, 2, 1, 3)
    gradient, image = pl.pallas_call(
        functools.partial(main_kernel, nd, ntr, nchunk),
        out_shape=(
            jax.ShapeDtypeStruct((depth, ncell), f32),
            jax.ShapeDtypeStruct((depth, traces), f32),
        ),
        in_specs=[anywhere] * 7,
        out_specs=(vmem, vmem),
        scratch_shapes=[
            pltpu.SMEM((groups,), jnp.int32),
            V((taps, angles), f32),
            V((1, angles), f32),
            V((depth, traces), f32),
            V(slow.shape, f32),
            V((depth, traces, angles), bf16),
            V((depth, traces, angles), bf16),
            V((3, 8, angles), f32),
            V((depth, LANES), f32),
            V((depth, 24, LANES), f32),
            V((depth, traces), f32),
            V((depth, traces), f32),
        ]
        + [V((depth, nedge), f32)] * 6
        + [
            V((nedge, traces), bf16),
            V((traces, LANES), bf16),
            V((nedge, LANES), bf16),
            V((nedge, LANES), bf16),
            V((depth, LANES), f32),
            V((near, 8, LANES), f32),
            V((2, depth, LANES), f32),
            V((side - 2, 8, LANES), f32),
            V((depth, LANES), f32),
            V((2, depth, LANES), f32),
            V((side - 2, 8, LANES), f32),
            V((depth, LANES), f32),
            V((near, 8, LANES), f32),
            V((8, LANES), f32),
            V((ntr, 8, LANES), f32),
            V((8, LANES), f32),
            V((ntr, 8, LANES), f32),
            V((depth, total), bf16),
            V((depth, total), bf16),
            V((depth, total), bf16),
            V((WIDE, total), bf16),
            V((ncell // WIDE, WIDE), f32),
            dma((4,)),
            dma,
            dma((nchunk,)),
            dma((nchunk,)),
            dma((near,)),
            dma((near,)),
            dma((side,)),
            dma((side,)),
            dma((side,)),
            dma((side,)),
            dma((near,)),
            dma((near,)),
            dma((ntr,)),
            dma((ntr,)),
            dma((ntr,)),
            dma((ntr,)),
        ],
        compiler_params=pltpu.CompilerParams(
            collective_id=0, has_side_effects=True, vmem_limit_bytes=VMEM_LIMIT
        ),
        name="radargram",
    )(slow, cell_of_group, taper.T, secant.reshape(1, angles), primary, quadrature, observed)
    return image, gradient


VMEM_LIMIT = 63 * 1024 * 1024


def solution(mesh):
    in_specs = (
        P("depth", None),
        P("track"),
        P(),
        P(),
        P("depth", "track", None),
        P("depth", "track", None),
        P("depth", "track"),
    )
    out_specs = (P("depth", "track"), P("depth", None))
    nd = mesh.shape["depth"]
    ntr = mesh.shape["track"]
    return jax.shard_map(
        functools.partial(on_device, nd, ntr), mesh=mesh, in_specs=in_specs, out_specs=out_specs, check_vma=False
    )
```

```python
import functools
import math

import jax
import jax.numpy as jnp
from jax import lax
from jax.experimental import pallas as pl
from jax.experimental.pallas import tpu as pltpu
from jax.sharding import PartitionSpec as P

OMEGA = 0.25
GROUP = 32
LANES = 128
MESH = pl.DeviceIdType.MESH

SIN = (4.442882919178189, -7.308245695274183, 3.6063544029247794, -0.8461128632742358, 0.10982698821149484)
COS = (1.4142134964903517, -6.978850985165349, 5.739461140914948, -1.8835629076104397, 0.310698190958135)

f32 = jnp.float32
bf16 = jnp.bfloat16


def horner(coefs, u):
    value = coefs[-1] * u + coefs[-2]
    for c in coefs[-3::-1]:
        value = value * u + c
    return value


def cos_sin(turns):
    r = turns - jnp.round(turns)
    u = r * r
    s = r * horner(SIN, u)
    c = horner(COS, u)
    return 1.0 - s * s, s * c


def iota(shape, dim):
    return lax.broadcasted_iota(jnp.int32, shape, dim)


def nt(a, b):
    return lax.dot_general(a, b, (((1,), (1,)), ((), ())), preferred_element_type=f32)


def nn(a, b):
    return lax.dot_general(a, b, (((1,), (0,)), ((), ())), preferred_element_type=f32)


def split3(x):
    high = x.astype(bf16).astype(f32)
    rest = x - high
    mid = rest.astype(bf16).astype(f32)
    return jnp.concatenate([high, mid, rest - mid], axis=0).astype(bf16)


def joined3(y):
    n = y.shape[0] // 3
    return y[:n] + y[n : 2 * n] + y[2 * n :]


def one_hot(mask):
    return jnp.where(mask, 1.0, 0.0).astype(bf16)


def peer_of(k, o, nd, nt_):
    d = lax.axis_index("depth")
    t = lax.axis_index("track")
    return (lax.rem(d + k, nd), lax.rem(t + o + nt_, nt_))


def near_copies(nd, nt_, src, tile, into, send, recv):
    return [
        pltpu.make_async_remote_copy(
            src.at[pl.ds(tile, 8)],
            into.at[k - 1],
            send.at[k - 1],
            recv.at[k - 1],
            device_id=peer_of(k, 0, nd, nt_),
            device_id_type=MESH,
        )
        for k in range(1, nd)
    ]


def side_copies(nd, nt_, src, tile, wide, narrow, send, recv):
    copies = []
    for i, o in enumerate((1, -1)):
        copies.append(
            pltpu.make_async_remote_copy(
                src, wide.at[i], send.at[i], recv.at[i], device_id=peer_of(0, o, nd, nt_), device_id_type=MESH
            )
        )
    for k in range(1, nd):
        for i, o in enumerate((1, -1)):
            at = 2 * (k - 1) + i
            copies.append(
                pltpu.make_async_remote_copy(
                    src.at[pl.ds(tile, 8)],
                    narrow.at[at],
                    send.at[2 + at],
                    recv.at[2 + at],
                    device_id=peer_of(k, o, nd, nt_),
                    device_id_type=MESH,
                )
            )
    return copies


WIDE = 256
PER_STEP = 8


def main_kernel(
    nd,
    ntr,
    nchunk,
    slow_hbm,
    cells_hbm,
    taper_hbm,
    secant_hbm,
    prim_hbm,
    quad_hbm,
    seen_hbm,
    grad,
    focused,
    cells,
    taper,
    secant,
    seen,
    slow,
    prim,
    quad,
    weights,
    line,
    spread,
    fint,
    bint,
    fedge,
    blo,
    bhi,
    fside,
    loside,
    hiside,
    edge_of,
    to_own,
    to_lo,
    to_hi,
    halo_a,
    near_a,
    wide_a,
    narrow_a,
    halo_b,
    wide_b,
    narrow_b,
    halo_c,
    near_c,
    mine,
    packets,
    below_mine,
    belows,
    ghigh,
    glow,
    block_of,
    place_of,
    rows_of,
    small_sem,
    slow_sem,
    prim_sem,
    quad_sem,
    send_a,
    recv_a,
    send_as,
    recv_as,
    send_b,
    recv_b,
    send_c,
    recv_c,
    send_p,
    recv_p,
    send_q,
    recv_q,
):
    d = lax.axis_index("depth")
    t = lax.axis_index("track")
    depth, traces, angles = prim.shape
    groups = traces // GROUP
    zc = depth // nchunk
    per = LANES // groups

    barrier = pltpu.get_barrier_semaphore()
    slow_copy = pltpu.make_async_copy(slow_hbm, slow, slow_sem)
    small = [
        pltpu.make_async_copy(cells_hbm, cells, small_sem.at[0]),
        pltpu.make_async_copy(taper_hbm, taper, small_sem.at[1]),
        pltpu.make_async_copy(secant_hbm, secant, small_sem.at[2]),
        pltpu.make_async_copy(seen_hbm, seen, small_sem.at[3]),
    ]
    small[0].start()
    slow_copy.start()

    @pl.loop(1, ntr)
    def _(k):
        pl.semaphore_signal(barrier, inc=1, device_id=(d, lax.rem(t + k, ntr)), device_id_type=MESH)

    for k in range(1, nd):
        for o in (-1, 0, 1):
            pl.semaphore_signal(barrier, inc=1, device_id=peer_of(k, o, nd, ntr), device_id_type=MESH)
    for copy in small[1:]:
        copy.start()

    def chunk_copies(i):
        rows = pl.ds(i * zc, zc)
        return (
            pltpu.make_async_copy(prim_hbm.at[rows], prim.at[rows], prim_sem.at[i]),
            pltpu.make_async_copy(quad_hbm.at[rows], quad.at[rows], quad_sem.at[i]),
        )

    mine_lane = iota((depth, LANES), 1)
    zrow = iota((depth, LANES), 0)
    small[0].wait()
    slow_copy.wait()

    @pl.loop(0, nchunk)
    def _(i):
        for copy in chunk_copies(i):
            copy.start()

    own = jnp.zeros((depth, LANES), f32)
    for g in range(groups):
        c = cells[g]
        block = slow[:, lax.div(c, LANES)].reshape(depth, LANES)
        column = jnp.sum(jnp.where(mine_lane == lax.rem(c, LANES), block, 0.0), axis=1, keepdims=True)
        own = jnp.where(mine_lane == g, column, own)
    s = 1
    while s < depth:
        own = own + jnp.where(zrow >= s, pltpu.roll(own, s, 0), 0.0)
        s *= 2
    halo_a[...] = own

    pl.semaphore_wait(barrier, ntr - 1 + 3 * (nd - 1))
    near = near_copies(nd, ntr, halo_a, depth - 8, near_a, send_a, recv_a)
    side_a = side_copies(nd, ntr, halo_a, depth - 8, wide_a, narrow_a, send_as, recv_as)
    for copy in near + side_a:
        copy.start()

    for copy in small[1:]:
        copy.wait()
    taps = taper[...]
    sec = secant[...] * OMEGA
    row = iota((8, angles), 0)
    nlo = jnp.where(row < 4, 4 - row, 12 - row)
    wlo = jnp.zeros((8, angles), f32)
    whi = jnp.zeros((8, angles), f32)
    for k in range(taper.shape[0]):
        tap = jnp.broadcast_to(taps[k : k + 1, :] * sec, (8, angles))
        wlo = wlo + jnp.where(k < nlo, tap, 0.0)
        whi = whi + jnp.where(k < nlo, 0.0, tap)
    weights[0] = wlo
    weights[1] = whi
    weights[2] = jnp.broadcast_to(jnp.sum(taps, axis=0, keepdims=True) * sec, (8, angles))

    nedge = groups * 8
    e = iota((nedge, traces), 0)
    x = iota((nedge, traces), 1)
    i = lax.rem(e, 8)
    at = lax.rem(lax.div(e, 8) * GROUP + jnp.where(i < 4, i, i - 8) + traces, traces)
    edge_of[...] = one_hot(at == x)
    to_own[...] = one_hot(lax.div(iota((traces, LANES), 0), GROUP) == iota((traces, LANES), 1))
    eb = iota((nedge, LANES), 0)
    el = iota((nedge, LANES), 1)
    bi = lax.div(eb, 8)
    behind_row = lax.rem(eb, 8) < 4
    to_lo[...] = one_hot(jnp.where(bi > 0, bi - 1, jnp.where(behind_row, groups, groups - 1)) == el)
    to_hi[...] = one_hot(jnp.where((bi > 0) | behind_row, bi, groups + 1) == el)
    seen_edge = joined3(nt(split3(seen[...]), edge_of[...]))

    for copy in near:
        copy.wait()

    def near_total(into, rowi, up):
        acc = jnp.zeros((1, LANES), f32)
        for k in range(1, nd):
            acc = acc + jnp.where((k <= d) if up else (k > d), into[k - 1, rowi : rowi + 1, :], 0.0)
        return acc

    def side_total(i, rowi, narrow, up):
        acc = jnp.zeros((1, LANES), f32)
        for k in range(1, nd):
            use = (k <= d) if up else (k > d)
            acc = acc + jnp.where(use, narrow[2 * (k - 1) + i, rowi : rowi + 1, :], 0.0)
        return acc

    turn = 1.0 / (2.0 * math.pi)
    line[...] = (own + near_total(near_a, 7, True)) * turn

    def spread_rows(first, count):
        diagonal = iota((count, LANES), 0) + first == iota((count, LANES), 1)

        @pl.loop(0, depth, unroll=8)
        def _(z):
            lines = jnp.broadcast_to(line[pl.ds(z, 1), :], (count, LANES))
            spread[z, first : first + count, :] = jnp.broadcast_to(
                jnp.sum(jnp.where(diagonal, lines, 0.0), axis=1, keepdims=True), (count, LANES)
            )

    spread_rows(0, groups)

    sub = iota((8, angles), 0)
    upper = sub < 4
    sub128 = iota((8, LANES), 0)
    lane128 = iota((8, LANES), 1)
    place = lax.rem(lane128, 8) == sub128
    half = 256
    own_group = sub == lax.div(iota((8, half), 1), GROUP)

    def splat(z, r):
        return jnp.broadcast_to(spread[z, r : r + 1, :], (8, LANES))

    def edge_sums(z, b, clo, chi):
        clo = jnp.concatenate([clo] * (angles // LANES), axis=1)
        chi = jnp.concatenate([chi] * (angles // LANES), axis=1)

        def edge_rows(ref):
            behind = ref[z, GROUP * b : GROUP * b + 8, :].astype(f32)
            stop = GROUP * b if b else traces
            before = ref[z, stop - 8 : stop, :].astype(f32)
            return jnp.where(upper, behind, before)

        pe = edge_rows(prim)
        qe = edge_rows(quad)
        wlo = weights[0]
        whi = weights[1]
        c, s = cos_sin(wlo * clo + whi * chi)
        g = qe * c - pe * s
        return [jnp.sum(v, axis=1, keepdims=True) for v in (pe * c + qe * s, g * wlo, g * whi)]

    def each_depth(z):
        for h in range(traces // half):
            first = h * half // GROUP
            c8 = spread[z, first : first + 8, :]
            w = weights[2]
            c, s = cos_sin(w * jnp.concatenate([c8] * (angles // LANES), axis=1))
            wc = w * c
            ws = w * s

            def pair(v):
                return [v, v - v.astype(bf16).astype(f32)]

            lhs_p = jnp.concatenate(pair(c) + pair(-ws), axis=0).astype(bf16)
            lhs_q = jnp.concatenate(pair(s) + pair(wc), axis=0).astype(bf16)
            rows = pl.ds(h * half, half)
            out = nt(lhs_p, prim[z, rows, :]) + nt(lhs_q, quad[z, rows, :])
            fsum = jnp.where(own_group, out[0:8] + out[8:16], 0.0)
            bsum = jnp.where(own_group, out[16:24] + out[24:32], 0.0)
            fint[pl.ds(z, 1), rows] = jnp.sum(fsum, axis=0, keepdims=True)
            bint[pl.ds(z, 1), rows] = jnp.sum(bsum, axis=0, keepdims=True)
        accs = [jnp.zeros((8, LANES), f32)] * 3
        for b in range(1, groups):
            here = lax.div(lane128, 8) == b
            found = edge_sums(z, b, splat(z, b - 1), splat(z, b))
            accs = [jnp.where(here, v, acc) for v, acc in zip(found, accs)]
        for acc, ref in zip(accs, (fedge, blo, bhi)):
            ref[pl.ds(z, 1), :] = jnp.sum(jnp.where(place, acc, 0.0), axis=0, keepdims=True)

    def outer_edge(z):
        clo = jnp.where(sub128 < 4, splat(z, groups), splat(z, groups - 1))
        chi = jnp.where(sub128 < 4, splat(z, 0), splat(z, groups + 1))
        found = edge_sums(z, 0, clo, chi)
        for v, ref in zip(found, (fside, loside, hiside)):
            picked = jnp.where(place & (lane128 < 8), v, 0.0)
            ref[pl.ds(z, 1), :] = jnp.sum(picked, axis=0, keepdims=True)

    @pl.loop(0, nchunk // 2)
    def _(i):
        for copy in chunk_copies(i):
            copy.wait()

        @pl.loop(0, zc, unroll=UNROLL)
        def _(j):
            each_depth(i * zc + j)

    for i in range(nchunk // 2, nchunk):
        for copy in chunk_copies(i):
            copy.wait()

    for copy in side_a:
        copy.wait()
    left = jnp.where(t > 0, wide_a[0] + side_total(0, 7, narrow_a, True), 0.0) * turn
    right = jnp.where(t < ntr - 1, wide_a[1] + side_total(1, 7, narrow_a, True), 0.0) * turn
    outer = jnp.where(mine_lane == groups, pltpu.roll(left, 1, 1), 0.0)
    line[...] = jnp.where(mine_lane == groups + 1, pltpu.roll(right, groups + 1, 1), outer)
    spread_rows(groups, 8)

    @pl.loop(0, depth, unroll=8)
    def _(z):
        outer_edge(z)

    def suffix(v):
        s = 1
        while s < depth:
            v = v + jnp.where(zrow < depth - s, pltpu.roll(v, depth - s, 0), 0.0)
            s *= 2
        return v

    resid = fside[...] - seen_edge
    to_left = jnp.sum(jnp.where(mine_lane < 4, resid * loside[...], 0.0), axis=1, keepdims=True)
    to_right = jnp.sum(
        jnp.where((mine_lane >= 4) & (mine_lane < 8), resid * hiside[...], 0.0), axis=1, keepdims=True
    )
    halo_b[...] = suffix(
        jnp.where(mine_lane == groups, to_left, jnp.where(mine_lane == groups + 1, to_right, 0.0))
    )
    side_b = side_copies(nd, ntr, halo_b, 0, wide_b, narrow_b, send_b, recv_b)
    for copy in side_b:
        copy.start()

    @pl.loop(depth // 2, depth, unroll=UNROLL)
    def _(z):
        each_depth(z)

    xoff = lax.rem(iota((depth, traces), 1), GROUP)
    inner = (xoff >= 4) & (xoff < GROUP - 4)
    term = jnp.where(inner, (fint[...] - seen[...]) * bint[...], 0.0)
    edge = fedge[...] + fside[...]
    resid = edge - seen_edge
    sums = joined3(nn(split3(term), to_own[...]))
    sums = sums + joined3(nn(split3(resid * (blo[...] + loside[...])), to_lo[...]))
    sums = sums + joined3(nn(split3(resid * (bhi[...] + hiside[...])), to_hi[...]))
    sums = suffix(sums)
    halo_c[...] = sums
    near = near_copies(nd, ntr, halo_c, 0, near_c, send_c, recv_c)
    for copy in near:
        copy.start()

    for copy in side_b:
        copy.wait()
    left = jnp.where(t > 0, wide_b[0] + side_total(0, 0, narrow_b, False), 0.0)
    right = jnp.where(t < ntr - 1, wide_b[1] + side_total(1, 0, narrow_b, False), 0.0)
    grads = jnp.where(mine_lane < groups, sums, 0.0)
    grads = grads + jnp.where(mine_lane == 0, pltpu.roll(left, LANES - groups - 1, 1), 0.0)
    grads = grads + jnp.where(mine_lane == groups - 1, pltpu.roll(right, LANES - 1, 1), 0.0)
    packet = jnp.zeros((8, LANES), f32)
    for g in range(groups):
        packet = jnp.where(lane128 == 4 * groups + g, cells[g].astype(f32), packet)
    for q in range(depth // 8):
        block = grads[8 * q : 8 * q + 8]
        packet = packet + (pltpu.roll(block, groups * q, 1) if q else block)
    shift = groups * lax.rem(t, per)
    packet = pltpu.roll(packet, shift, 1)
    mine[...] = packet
    packets[t] = packet

    def track_copy(k, src, into, send, recv, sender):
        return pltpu.make_async_remote_copy(
            src,
            into.at[sender],
            send.at[k],
            recv.at[k],
            device_id=(d, lax.rem(t + k, ntr)),
            device_id_type=MESH,
        )

    def sent(k, src, into, send, recv):
        return track_copy(k, src, into, send, recv, t)

    def arrived(k, src, into, send, recv):
        return track_copy(k, src, into, send, recv, lax.rem(t + ntr - k, ntr))

    first = (mine, packets, send_p, recv_p)
    second = (below_mine, belows, send_q, recv_q)

    @pl.loop(1, ntr)
    def _(k):
        sent(k, *first).start()

    for copy in near:
        copy.wait()
    below = jnp.where(lane128 < groups, jnp.broadcast_to(near_total(near_c, 0, False), (8, LANES)), 0.0)
    below = pltpu.roll(below, shift, 1)
    below_mine[...] = below
    belows[t] = below

    @pl.loop(1, ntr)
    def _(k):
        sent(k, *second).start()

    focused[...] = jnp.where(inner, fint[...], joined3(nn(split3(edge), edge_of[...])))

    @pl.loop(1, ntr)
    def _(k):
        arrived(k, *first).wait_recv()

    chunk = lax.div(lane128, groups)
    for col in range(ntr // per):
        parts = []
        for q in range(depth // 8 + 1):
            acc = jnp.zeros((8, LANES), f32)
            for j in range(per):
                acc = jnp.where(chunk == (q + j) % per, packets[col * per + j], acc)
            parts.append(pltpu.roll(acc, LANES - groups * q, 1) if q else acc)
        lanes = pl.ds(col * LANES, LANES)
        g = jnp.concatenate(parts[:-1], axis=0)
        high = g.astype(bf16)
        ghigh[:, lanes] = high
        glow[:, lanes] = (g - high.astype(f32)).astype(bf16)
        cell = parts[-1][0:1]
        block = jnp.floor(cell * (1.0 / WIDE))
        block_of[:, lanes] = jnp.broadcast_to(block, (depth, LANES)).astype(bf16)
        place_of[:, lanes] = one_hot(iota((WIDE, LANES), 0).astype(f32) == cell - block * WIDE)

    nblock = grad.shape[1] // WIDE

    @pl.loop(0, nblock // PER_STEP)
    def _(step):
        highs = []
        lows = []
        for j in range(PER_STEP):
            mask = block_of[...] == (step * PER_STEP + j).astype(bf16)
            highs.append(jnp.where(mask, ghigh[...], jnp.zeros((), bf16)))
            lows.append(jnp.where(mask, glow[...], jnp.zeros((), bf16)))
        out = nt(jnp.concatenate(highs, axis=0), place_of[...]) + nt(jnp.concatenate(lows, axis=0), place_of[...])
        out = jnp.concatenate([out[depth * j : depth * (j + 1)] for j in range(PER_STEP)], axis=1)
        wide = PER_STEP * WIDE
        grad[:, pl.ds(pl.multiple_of(step * wide, wide), wide)] = out

    @pl.loop(1, ntr)
    def _(k):
        arrived(k, *second).wait_recv()

    cols = []
    for col in range(ntr // per):
        acc = belows[col * per, 0:1, :]
        for j in range(1, per):
            acc = acc + belows[col * per + j, 0:1, :]
        cols.append(acc)
    below = jnp.broadcast_to(jnp.concatenate(cols, axis=1), (nblock, ntr * groups))
    blocks = jnp.broadcast_to(block_of[...].astype(f32)[0:1], (nblock, ntr * groups))
    spread_below = jnp.where(blocks == iota((nblock, ntr * groups), 0).astype(f32), below, 0.0)
    rows_of[...] = joined3(nt(split3(spread_below), place_of[...]))

    @pl.loop(0, nblock, unroll=8)
    def _(j):
        lanes = pl.ds(pl.multiple_of(j * WIDE, WIDE), WIDE)
        grad[:, lanes] = grad[:, lanes] + jnp.broadcast_to(rows_of[pl.ds(j, 1), :], (depth, WIDE))

    @pl.loop(1, ntr)
    def _(k):
        sent(k, *first).wait_send()
        sent(k, *second).wait_send()


UNROLL = 2


def on_device(nd, ntr, slowness_cells, cell_of_group, taper, secant, primary, quadrature, observed):
    depth, traces, angles = primary.shape
    taps = taper.shape[1]
    ncell = slowness_cells.shape[1]
    groups = cell_of_group.shape[0]
    nedge = groups * 8
    total = ntr * groups
    nchunk = 8
    vmem = pl.BlockSpec(memory_space=pltpu.VMEM)
    anywhere = pl.BlockSpec(memory_space=pl.ANY)
    near = nd - 1
    side = 2 * nd
    dma = pltpu.SemaphoreType.DMA
    V = pltpu.VMEM
    slow = slowness_cells.reshape(depth // 8, 8, ncell // LANES, LANES).transpose(0, 2, 1, 3)
    gradient, image = pl.pallas_call(
        functools.partial(main_kernel, nd, ntr, nchunk),
        out_shape=(
            jax.ShapeDtypeStruct((depth, ncell), f32),
            jax.ShapeDtypeStruct((depth, traces), f32),
        ),
        in_specs=[anywhere] * 7,
        out_specs=(vmem, vmem),
        scratch_shapes=[
            pltpu.SMEM((groups,), jnp.int32),
            V((taps, angles), f32),
            V((1, angles), f32),
            V((depth, traces), f32),
            V(slow.shape, f32),
            V((depth, traces, angles), bf16),
            V((depth, traces, angles), bf16),
            V((3, 8, angles), f32),
            V((depth, LANES), f32),
            V((depth, 24, LANES), f32),
            V((depth, traces), f32),
            V((depth, traces), f32),
        ]
        + [V((depth, nedge), f32)] * 6
        + [
            V((nedge, traces), bf16),
            V((traces, LANES), bf16),
            V((nedge, LANES), bf16),
            V((nedge, LANES), bf16),
            V((depth, LANES), f32),
            V((near, 8, LANES), f32),
            V((2, depth, LANES), f32),
            V((side - 2, 8, LANES), f32),
            V((depth, LANES), f32),
            V((2, depth, LANES), f32),
            V((side - 2, 8, LANES), f32),
            V((depth, LANES), f32),
            V((near, 8, LANES), f32),
            V((8, LANES), f32),
            V((ntr, 8, LANES), f32),
            V((8, LANES), f32),
            V((ntr, 8, LANES), f32),
            V((depth, total), bf16),
            V((depth, total), bf16),
            V((depth, total), bf16),
            V((WIDE, total), bf16),
            V((ncell // WIDE, WIDE), f32),
            dma((4,)),
            dma,
            dma((nchunk,)),
            dma((nchunk,)),
            dma((near,)),
            dma((near,)),
            dma((side,)),
            dma((side,)),
            dma((side,)),
            dma((side,)),
            dma((near,)),
            dma((near,)),
            dma((ntr,)),
            dma((ntr,)),
            dma((ntr,)),
            dma((ntr,)),
        ],
        compiler_params=pltpu.CompilerParams(
            collective_id=0, has_side_effects=True, vmem_limit_bytes=VMEM_LIMIT
        ),
        name="radargram",
    )(
        *[
            pltpu.with_memory_space_constraint(v, pltpu.HBM)
            for v in (slow, cell_of_group, taper.T, secant.reshape(1, angles), primary, quadrature, observed)
        ]
    )
    gradient, image = pl.pallas_call(
        hand_out,
        out_shape=(
            jax.ShapeDtypeStruct((depth, ncell), f32),
            jax.ShapeDtypeStruct((depth, traces), f32),
        ),
        in_specs=[anywhere] * 2,
        out_specs=(anywhere, anywhere),
        scratch_shapes=[dma((2,))],
        compiler_params=pltpu.CompilerParams(vmem_limit_bytes=1024 * 1024),
        name="hand_out",
    )(gradient, image)
    return image, gradient


def hand_out(grad, image, grad_out, image_out, sems):
    copies = [
        pltpu.make_async_copy(grad, grad_out, sems.at[0]),
        pltpu.make_async_copy(image, image_out, sems.at[1]),
    ]
    for copy in copies:
        copy.start()
    for copy in copies:
        copy.wait()


VMEM_LIMIT = 40 * 1024 * 1024


def solution(mesh):
    in_specs = (
        P("depth", None),
        P("track"),
        P(),
        P(),
        P("depth", "track", None),
        P("depth", "track", None),
        P("depth", "track"),
    )
    out_specs = (P("depth", "track"), P("depth", None))
    nd = mesh.shape["depth"]
    ntr = mesh.shape["track"]
    return jax.shard_map(
        functools.partial(on_device, nd, ntr), mesh=mesh, in_specs=in_specs, out_specs=out_specs, check_vma=False
    )
```

```python
import functools
import math

import jax
import jax.numpy as jnp
from jax import lax
from jax.experimental import pallas as pl
from jax.experimental.pallas import tpu as pltpu
from jax.sharding import PartitionSpec as P

OMEGA = 0.25
GROUP = 32
LANES = 128
MESH = pl.DeviceIdType.MESH

SIN = (4.442882919178189, -7.308245695274183, 3.6063544029247794, -0.8461128632742358, 0.10982698821149484)
COS = (1.4142134964903517, -6.978850985165349, 5.739461140914948, -1.8835629076104397, 0.310698190958135)

f32 = jnp.float32
bf16 = jnp.bfloat16


def horner(coefs, u):
    value = coefs[-1] * u + coefs[-2]
    for c in coefs[-3::-1]:
        value = value * u + c
    return value


def cos_sin(turns):
    r = turns - jnp.round(turns)
    u = r * r
    s = r * horner(SIN, u)
    c = horner(COS, u)
    return 1.0 - s * s, s * c


def iota(shape, dim):
    return lax.broadcasted_iota(jnp.int32, shape, dim)


def nt(a, b):
    return lax.dot_general(a, b, (((1,), (1,)), ((), ())), preferred_element_type=f32)


def nn(a, b):
    return lax.dot_general(a, b, (((1,), (0,)), ((), ())), preferred_element_type=f32)


def split3(x):
    high = x.astype(bf16).astype(f32)
    rest = x - high
    mid = rest.astype(bf16).astype(f32)
    return jnp.concatenate([high, mid, rest - mid], axis=0).astype(bf16)


def joined3(y):
    n = y.shape[0] // 3
    return y[:n] + y[n : 2 * n] + y[2 * n :]


def one_hot(mask):
    return jnp.where(mask, 1.0, 0.0).astype(bf16)


def peer_of(k, o, nd, nt_):
    d = lax.axis_index("depth")
    t = lax.axis_index("track")
    return (lax.rem(d + k, nd), lax.rem(t + o + nt_, nt_))


def near_copies(nd, nt_, src, tile, into, send, recv):
    return [
        pltpu.make_async_remote_copy(
            src.at[pl.ds(tile, 8)],
            into.at[pl.ds(8 * (k - 1), 8)],
            send,
            recv,
            device_id=peer_of(k, 0, nd, nt_),
            device_id_type=MESH,
        )
        for k in range(1, nd)
    ]


def side_copies(nd, nt_, src, tile, into, send, recv):
    depth = src.shape[0]
    copies = []
    for i, o in enumerate((1, -1)):
        copies.append(
            pltpu.make_async_remote_copy(
                src,
                into.at[pl.ds(i * depth, depth)],
                send,
                recv,
                device_id=peer_of(0, o, nd, nt_),
                device_id_type=MESH,
            )
        )
        for k in range(1, nd):
            copies.append(
                pltpu.make_async_remote_copy(
                    src.at[pl.ds(tile, 8)],
                    into.at[pl.ds(2 * depth + 8 * (2 * (k - 1) + i), 8)],
                    send,
                    recv,
                    device_id=peer_of(k, o, nd, nt_),
                    device_id_type=MESH,
                )
            )
    return copies


def wait_all(into, send, recv, nd, nt_):
    copy = pltpu.make_async_remote_copy(
        into, into, send, recv, device_id=peer_of(1, 0, nd, nt_), device_id_type=MESH
    )
    copy.wait_recv()
    copy.wait_send()


WIDE = 256
PER_STEP = 16


def main_kernel(
    nd,
    ntr,
    nchunk,
    slow_hbm,
    cells_hbm,
    taper_hbm,
    secant_hbm,
    prim_hbm,
    quad_hbm,
    seen_hbm,
    grad,
    focused,
    cells,
    taper,
    secant,
    seen,
    slow,
    prim,
    quad,
    weights,
    line,
    spread,
    fint,
    bint,
    fedge,
    blo,
    bhi,
    fside,
    loside,
    hiside,
    edge_of,
    to_own,
    to_lo,
    to_hi,
    halo_a,
    near_a,
    side_a,
    halo_b,
    side_b,
    halo_c,
    near_c,
    cells_mine,
    cell_rows,
    mine,
    packets,
    below_mine,
    belows,
    ghigh,
    glow,
    block_of,
    place_of,
    rows_of,
    small_sem,
    slow_sem,
    prim_sem,
    quad_sem,
    send_a,
    recv_a,
    send_as,
    recv_as,
    send_cells,
    recv_cells,
    send_b,
    recv_b,
    send_c,
    recv_c,
    send_p,
    recv_p,
    send_q,
    recv_q,
):
    d = lax.axis_index("depth")
    t = lax.axis_index("track")
    depth, traces, angles = prim.shape
    groups = traces // GROUP
    zc = depth // nchunk
    per = LANES // groups

    barrier = pltpu.get_barrier_semaphore()
    slow_copy = pltpu.make_async_copy(slow_hbm, slow, slow_sem)
    small = [
        pltpu.make_async_copy(cells_hbm, cells, small_sem.at[0]),
        pltpu.make_async_copy(taper_hbm, taper, small_sem.at[1]),
        pltpu.make_async_copy(secant_hbm, secant, small_sem.at[2]),
        pltpu.make_async_copy(seen_hbm, seen, small_sem.at[3]),
    ]
    small[0].start()
    slow_copy.start()

    @pl.loop(1, ntr)
    def _(k):
        pl.semaphore_signal(barrier, inc=1, device_id=(d, lax.rem(t + k, ntr)), device_id_type=MESH)

    for k in range(1, nd):
        for o in (-1, 0, 1):
            pl.semaphore_signal(barrier, inc=1, device_id=peer_of(k, o, nd, ntr), device_id_type=MESH)
    for copy in small[1:]:
        copy.start()

    def chunk_copies(i):
        rows = pl.ds(i * zc, zc)
        return (
            pltpu.make_async_copy(prim_hbm.at[rows], prim.at[rows], prim_sem.at[i]),
            pltpu.make_async_copy(quad_hbm.at[rows], quad.at[rows], quad_sem.at[i]),
        )

    mine_lane = iota((depth, LANES), 1)
    zrow = iota((depth, LANES), 0)
    small[0].wait()
    slow_copy.wait()

    @pl.loop(0, nchunk)
    def _(i):
        for copy in chunk_copies(i):
            copy.start()

    own = jnp.zeros((depth, LANES), f32)
    for g in range(groups):
        c = cells[g]
        block = slow[:, lax.div(c, LANES)].reshape(depth, LANES)
        column = jnp.sum(jnp.where(mine_lane == lax.rem(c, LANES), block, 0.0), axis=1, keepdims=True)
        own = jnp.where(mine_lane == g, column, own)
    s = 1
    while s < depth:
        own = own + jnp.where(zrow >= s, pltpu.roll(own, s, 0), 0.0)
        s *= 2
    halo_a[...] = own

    pl.semaphore_wait(barrier, ntr - 1 + 3 * (nd - 1))
    for copy in near_copies(nd, ntr, halo_a, depth - 8, near_a, send_a, recv_a):
        copy.start()
    for copy in side_copies(nd, ntr, halo_a, depth - 8, side_a, send_as, recv_as):
        copy.start()

    lane1 = iota((1, LANES), 1)
    shift = groups * lax.rem(t, per)
    row = jnp.zeros((1, LANES), f32)
    for g in range(groups):
        row = jnp.where(lane1 == shift + g, cells[g].astype(f32), row)
    cells_mine[...] = row
    cell_rows[t] = row

    def to_track(k, src, into, send, recv):
        pltpu.make_async_remote_copy(
            src,
            into.at[t],
            send,
            recv,
            device_id=(d, lax.rem(t + k, ntr)),
            device_id_type=MESH,
        ).start()

    @pl.loop(1, ntr)
    def _(k):
        to_track(k, cells_mine, cell_rows, send_cells, recv_cells)

    def others(ref):
        return ref.at[pl.ds(0, ntr - 1)]

    def track_row(ref, col):
        acc = ref[col * per]
        for j in range(1, per):
            acc = acc + ref[col * per + j]
        return acc

    for copy in small[1:]:
        copy.wait()
    taps = taper[...]
    sec = secant[...] * OMEGA
    row = iota((8, angles), 0)
    nlo = jnp.where(row < 4, 4 - row, 12 - row)
    wlo = jnp.zeros((8, angles), f32)
    whi = jnp.zeros((8, angles), f32)
    for k in range(taper.shape[0]):
        tap = jnp.broadcast_to(taps[k : k + 1, :] * sec, (8, angles))
        wlo = wlo + jnp.where(k < nlo, tap, 0.0)
        whi = whi + jnp.where(k < nlo, 0.0, tap)
    weights[0] = wlo
    weights[1] = whi
    weights[2] = jnp.broadcast_to(jnp.sum(taps, axis=0, keepdims=True) * sec, (8, angles))

    nedge = groups * 8
    e = iota((nedge, traces), 0)
    x = iota((nedge, traces), 1)
    i = lax.rem(e, 8)
    at = lax.rem(lax.div(e, 8) * GROUP + jnp.where(i < 4, i, i - 8) + traces, traces)
    edge_of[...] = one_hot(at == x)
    to_own[...] = one_hot(lax.div(iota((traces, LANES), 0), GROUP) == iota((traces, LANES), 1))
    eb = iota((nedge, LANES), 0)
    el = iota((nedge, LANES), 1)
    bi = lax.div(eb, 8)
    behind_row = lax.rem(eb, 8) < 4
    to_lo[...] = one_hot(jnp.where(bi > 0, bi - 1, jnp.where(behind_row, groups, groups - 1)) == el)
    to_hi[...] = one_hot(jnp.where((bi > 0) | behind_row, bi, groups + 1) == el)
    seen_edge = joined3(nt(split3(seen[...]), edge_of[...]))

    wait_all(near_a, send_a, recv_a, nd, ntr)

    def near_total(into, rowi, up):
        acc = jnp.zeros((1, LANES), f32)
        for k in range(1, nd):
            at = 8 * (k - 1) + rowi
            acc = acc + jnp.where((k <= d) if up else (k > d), into[at : at + 1, :], 0.0)
        return acc

    def side_total(i, rowi, into, up):
        acc = into[i * depth : (i + 1) * depth, :]
        for k in range(1, nd):
            use = (k <= d) if up else (k > d)
            at = 2 * depth + 8 * (2 * (k - 1) + i) + rowi
            acc = acc + jnp.where(use, into[at : at + 1, :], 0.0)
        return acc

    turn = 1.0 / (2.0 * math.pi)
    line[...] = (own + near_total(near_a, 7, True)) * turn

    def spread_rows(first, count):
        diagonal = iota((count, LANES), 0) + first == iota((count, LANES), 1)

        @pl.loop(0, depth, unroll=8)
        def _(z):
            lines = jnp.broadcast_to(line[pl.ds(z, 1), :], (count, LANES))
            spread[z, first : first + count, :] = jnp.broadcast_to(
                jnp.sum(jnp.where(diagonal, lines, 0.0), axis=1, keepdims=True), (count, LANES)
            )

    spread_rows(0, groups)

    sub = iota((8, angles), 0)
    upper = sub < 4
    sub128 = iota((8, LANES), 0)
    lane128 = iota((8, LANES), 1)
    place = lax.rem(lane128, 8) == sub128
    half = 256
    own_group = sub == lax.div(iota((8, half), 1), GROUP)

    def splat(z, r):
        return jnp.broadcast_to(spread[z, r : r + 1, :], (8, LANES))

    def edge_sums(z, b, clo, chi):
        clo = jnp.concatenate([clo] * (angles // LANES), axis=1)
        chi = jnp.concatenate([chi] * (angles // LANES), axis=1)

        def edge_rows(ref):
            behind = ref[z, GROUP * b : GROUP * b + 8, :].astype(f32)
            stop = GROUP * b if b else traces
            before = ref[z, stop - 8 : stop, :].astype(f32)
            return jnp.where(upper, behind, before)

        pe = edge_rows(prim)
        qe = edge_rows(quad)
        wlo = weights[0]
        whi = weights[1]
        c, s = cos_sin(wlo * clo + whi * chi)
        g = qe * c - pe * s
        return [jnp.sum(v, axis=1, keepdims=True) for v in (pe * c + qe * s, g * wlo, g * whi)]

    def each_depth(z):
        for h in range(traces // half):
            first = h * half // GROUP
            c8 = spread[z, first : first + 8, :]
            w = weights[2]
            c, s = cos_sin(w * jnp.concatenate([c8] * (angles // LANES), axis=1))
            wc = w * c
            ws = w * s

            def pair(v):
                return [v, v - v.astype(bf16).astype(f32)]

            lhs_p = jnp.concatenate(pair(c) + pair(-ws), axis=0).astype(bf16)
            lhs_q = jnp.concatenate(pair(s) + pair(wc), axis=0).astype(bf16)
            rows = pl.ds(h * half, half)
            out = nt(lhs_p, prim[z, rows, :]) + nt(lhs_q, quad[z, rows, :])
            fsum = jnp.where(own_group, out[0:8] + out[8:16], 0.0)
            bsum = jnp.where(own_group, out[16:24] + out[24:32], 0.0)
            fint[pl.ds(z, 1), rows] = jnp.sum(fsum, axis=0, keepdims=True)
            bint[pl.ds(z, 1), rows] = jnp.sum(bsum, axis=0, keepdims=True)
        accs = [jnp.zeros((8, LANES), f32)] * 3
        for b in range(1, groups):
            here = lax.div(lane128, 8) == b
            found = edge_sums(z, b, splat(z, b - 1), splat(z, b))
            accs = [jnp.where(here, v, acc) for v, acc in zip(found, accs)]
        for acc, ref in zip(accs, (fedge, blo, bhi)):
            ref[pl.ds(z, 1), :] = jnp.sum(jnp.where(place, acc, 0.0), axis=0, keepdims=True)

    def outer_edge(z):
        clo = jnp.where(sub128 < 4, splat(z, groups), splat(z, groups - 1))
        chi = jnp.where(sub128 < 4, splat(z, 0), splat(z, groups + 1))
        found = edge_sums(z, 0, clo, chi)
        for v, ref in zip(found, (fside, loside, hiside)):
            picked = jnp.where(place & (lane128 < 8), v, 0.0)
            ref[pl.ds(z, 1), :] = jnp.sum(picked, axis=0, keepdims=True)

    @pl.loop(0, FIRST_CHUNKS)
    def _(i):
        for copy in chunk_copies(i):
            copy.wait()

        @pl.loop(0, zc, unroll=UNROLL)
        def _(j):
            each_depth(i * zc + j)

    @pl.loop(FIRST_CHUNKS, nchunk)
    def _(i):
        for copy in chunk_copies(i):
            copy.wait()

    wait_all(side_a, send_as, recv_as, nd, ntr)
    left = jnp.where(t > 0, side_total(0, 7, side_a, True), 0.0) * turn
    right = jnp.where(t < ntr - 1, side_total(1, 7, side_a, True), 0.0) * turn
    outer = jnp.where(mine_lane == groups, pltpu.roll(left, 1, 1), 0.0)
    line[...] = jnp.where(mine_lane == groups + 1, pltpu.roll(right, groups + 1, 1), outer)
    spread_rows(groups, 8)

    @pl.loop(0, depth, unroll=8)
    def _(z):
        outer_edge(z)

    def suffix(v):
        s = 1
        while s < depth:
            v = v + jnp.where(zrow < depth - s, pltpu.roll(v, depth - s, 0), 0.0)
            s *= 2
        return v

    resid = fside[...] - seen_edge
    to_left = jnp.sum(jnp.where(mine_lane < 4, resid * loside[...], 0.0), axis=1, keepdims=True)
    to_right = jnp.sum(
        jnp.where((mine_lane >= 4) & (mine_lane < 8), resid * hiside[...], 0.0), axis=1, keepdims=True
    )
    halo_b[...] = suffix(
        jnp.where(mine_lane == groups, to_left, jnp.where(mine_lane == groups + 1, to_right, 0.0))
    )
    for copy in side_copies(nd, ntr, halo_b, 0, side_b, send_b, recv_b):
        copy.start()

    wait_all(others(cell_rows), send_cells, recv_cells, nd, ntr)
    for col in range(ntr // per):
        lanes = pl.ds(col * LANES, LANES)
        cell = track_row(cell_rows, col)
        block = jnp.floor(cell * (1.0 / WIDE))
        block_of[:, lanes] = jnp.broadcast_to(block, (depth, LANES)).astype(bf16)
        place_of[:, lanes] = one_hot(iota((WIDE, LANES), 0).astype(f32) == cell - block * WIDE)

    @pl.loop(FIRST_CHUNKS * zc, depth, unroll=UNROLL)
    def _(z):
        each_depth(z)

    xoff = lax.rem(iota((depth, traces), 1), GROUP)
    inner = (xoff >= 4) & (xoff < GROUP - 4)
    term = jnp.where(inner, (fint[...] - seen[...]) * bint[...], 0.0)
    edge = fedge[...] + fside[...]
    resid = edge - seen_edge
    sums = joined3(nn(split3(term), to_own[...]))
    sums = sums + joined3(nn(split3(resid * (blo[...] + loside[...])), to_lo[...]))
    sums = sums + joined3(nn(split3(resid * (bhi[...] + hiside[...])), to_hi[...]))
    sums = suffix(sums)
    halo_c[...] = sums
    for copy in near_copies(nd, ntr, halo_c, 0, near_c, send_c, recv_c):
        copy.start()

    wait_all(side_b, send_b, recv_b, nd, ntr)
    left = jnp.where(t > 0, side_total(0, 0, side_b, False), 0.0)
    right = jnp.where(t < ntr - 1, side_total(1, 0, side_b, False), 0.0)
    grads = jnp.where(mine_lane < groups, sums, 0.0)
    grads = grads + jnp.where(mine_lane == 0, pltpu.roll(left, LANES - groups - 1, 1), 0.0)
    grads = grads + jnp.where(mine_lane == groups - 1, pltpu.roll(right, LANES - 1, 1), 0.0)
    packet = jnp.zeros((8, LANES), f32)
    for q in range(depth // 8):
        block = grads[8 * q : 8 * q + 8]
        packet = packet + (pltpu.roll(block, groups * q, 1) if q else block)
    packet = packet + pltpu.roll(pltpu.roll(packet, 4, 0), LANES // 2, 1)
    packet = pltpu.roll(packet, shift, 1)[0:4]
    mine[...] = packet
    packets[t] = packet

    @pl.loop(1, ntr)
    def _(k):
        to_track(k, mine, packets, send_p, recv_p)

    wait_all(near_c, send_c, recv_c, nd, ntr)
    below = pltpu.roll(
        jnp.broadcast_to(jnp.where(lane1 < groups, near_total(near_c, 0, False), 0.0), (8, LANES)), shift, 1
    )[0:1]
    below_mine[...] = below
    belows[t] = below

    @pl.loop(1, ntr)
    def _(k):
        to_track(k, below_mine, belows, send_q, recv_q)

    focused[...] = jnp.where(inner, fint[...], joined3(nn(split3(edge), edge_of[...])))
    wait_all(others(packets), send_p, recv_p, nd, ntr)

    chunk = lax.div(iota((4, LANES), 1), groups)
    for col in range(ntr // per):
        parts = []
        for c in range(per):
            acc = jnp.zeros((4, LANES), f32)
            for j in range(per):
                acc = jnp.where(chunk == (c + j) % per, packets[col * per + j], acc)
            parts.append(acc)
        lanes = pl.ds(col * LANES, LANES)
        nq = depth // 8
        pieces = []
        for q in range(nq):
            for h in range(2):
                c = q + nq * h
                both = jnp.concatenate([parts[c], parts[c]], axis=0)
                pieces.append(pltpu.roll(both, LANES - groups * c, 1) if c else both)
        low_rows = iota((8, LANES), 0) < 4
        g = jnp.concatenate(
            [jnp.where(low_rows, pieces[2 * q], pieces[2 * q + 1]) for q in range(nq)], axis=0
        )
        high = g.astype(bf16)
        ghigh[:, lanes] = high
        glow[:, lanes] = (g - high.astype(f32)).astype(bf16)

    nblock = grad.shape[1] // WIDE

    @pl.loop(0, nblock // PER_STEP)
    def _(step):
        highs = []
        lows = []
        for j in range(PER_STEP):
            mask = block_of[...] == (step * PER_STEP + j).astype(bf16)
            highs.append(jnp.where(mask, ghigh[...], jnp.zeros((), bf16)))
            lows.append(jnp.where(mask, glow[...], jnp.zeros((), bf16)))
        out = nt(jnp.concatenate(highs, axis=0), place_of[...]) + nt(jnp.concatenate(lows, axis=0), place_of[...])
        out = jnp.concatenate([out[depth * j : depth * (j + 1)] for j in range(PER_STEP)], axis=1)
        wide = PER_STEP * WIDE
        grad[:, pl.ds(pl.multiple_of(step * wide, wide), wide)] = out

    wait_all(others(belows), send_q, recv_q, nd, ntr)
    below = jnp.concatenate([track_row(belows, col) for col in range(ntr // per)], axis=1)
    below = jnp.broadcast_to(below, (nblock, ntr * groups))
    blocks = jnp.broadcast_to(block_of[...].astype(f32)[0:1], (nblock, ntr * groups))
    spread_below = jnp.where(blocks == iota((nblock, ntr * groups), 0).astype(f32), below, 0.0)
    rows_of[...] = joined3(nt(split3(spread_below), place_of[...]))

    @pl.loop(0, nblock, unroll=8)
    def _(j):
        lanes = pl.ds(pl.multiple_of(j * WIDE, WIDE), WIDE)
        grad[:, lanes] = grad[:, lanes] + jnp.broadcast_to(rows_of[pl.ds(j, 1), :], (depth, WIDE))


FIRST_CHUNKS = 2
UNROLL = 2


def on_device(nd, ntr, slowness_cells, cell_of_group, taper, secant, primary, quadrature, observed):
    depth, traces, angles = primary.shape
    taps = taper.shape[1]
    ncell = slowness_cells.shape[1]
    groups = cell_of_group.shape[0]
    nedge = groups * 8
    total = ntr * groups
    nchunk = 8
    vmem = pl.BlockSpec(memory_space=pltpu.VMEM)
    anywhere = pl.BlockSpec(memory_space=pl.ANY)
    near = nd - 1
    dma = pltpu.SemaphoreType.DMA
    V = pltpu.VMEM
    slow = slowness_cells.reshape(depth // 8, 8, ncell // LANES, LANES).transpose(0, 2, 1, 3)
    gradient, image = pl.pallas_call(
        functools.partial(main_kernel, nd, ntr, nchunk),
        out_shape=(
            jax.ShapeDtypeStruct((depth, ncell), f32),
            jax.ShapeDtypeStruct((depth, traces), f32),
        ),
        in_specs=[anywhere] * 7,
        out_specs=(vmem, vmem),
        scratch_shapes=[
            pltpu.SMEM((groups,), jnp.int32),
            V((taps, angles), f32),
            V((1, angles), f32),
            V((depth, traces), f32),
            V(slow.shape, f32),
            V((depth, traces, angles), bf16),
            V((depth, traces, angles), bf16),
            V((3, 8, angles), f32),
            V((depth, LANES), f32),
            V((depth, 24, LANES), f32),
            V((depth, traces), f32),
            V((depth, traces), f32),
        ]
        + [V((depth, nedge), f32)] * 6
        + [
            V((nedge, traces), bf16),
            V((traces, LANES), bf16),
            V((nedge, LANES), bf16),
            V((nedge, LANES), bf16),
            V((depth, LANES), f32),
            V((8 * near, LANES), f32),
            V((2 * depth + 16 * near, LANES), f32),
            V((depth, LANES), f32),
            V((2 * depth + 16 * near, LANES), f32),
            V((depth, LANES), f32),
            V((8 * near, LANES), f32),
            V((1, LANES), f32),
            V((ntr, 1, LANES), f32),
            V((4, LANES), f32),
            V((ntr, 4, LANES), f32),
            V((1, LANES), f32),
            V((ntr, 1, LANES), f32),
            V((depth, total), bf16),
            V((depth, total), bf16),
            V((depth, total), bf16),
            V((WIDE, total), bf16),
            V((ncell // WIDE, WIDE), f32),
            dma((4,)),
            dma,
            dma((nchunk,)),
            dma((nchunk,)),
        ]
        + [dma] * 14,
        compiler_params=pltpu.CompilerParams(
            collective_id=0, has_side_effects=True, vmem_limit_bytes=VMEM_LIMIT
        ),
        name="radargram",
    )(
        *[
            pltpu.with_memory_space_constraint(v, pltpu.HBM)
            for v in (slow, cell_of_group, taper.T, secant.reshape(1, angles), primary, quadrature, observed)
        ]
    )
    gradient, image = pl.pallas_call(
        hand_out,
        out_shape=(
            jax.ShapeDtypeStruct((depth, ncell), f32),
            jax.ShapeDtypeStruct((depth, traces), f32),
        ),
        in_specs=[anywhere] * 2,
        out_specs=(anywhere, anywhere),
        scratch_shapes=[dma((2,))],
        compiler_params=pltpu.CompilerParams(vmem_limit_bytes=1024 * 1024),
        name="hand_out",
    )(gradient, image)
    return image, gradient


def hand_out(grad, image, grad_out, image_out, sems):
    copies = [
        pltpu.make_async_copy(grad, grad_out, sems.at[0]),
        pltpu.make_async_copy(image, image_out, sems.at[1]),
    ]
    for copy in copies:
        copy.start()
    for copy in copies:
        copy.wait()


VMEM_LIMIT = 40 * 1024 * 1024


def solution(mesh):
    in_specs = (
        P("depth", None),
        P("track"),
        P(),
        P(),
        P("depth", "track", None),
        P("depth", "track", None),
        P("depth", "track"),
    )
    out_specs = (P("depth", "track"), P("depth", None))
    nd = mesh.shape["depth"]
    ntr = mesh.shape["track"]
    return jax.shard_map(
        functools.partial(on_device, nd, ntr), mesh=mesh, in_specs=in_specs, out_specs=out_specs, check_vma=False
    )
```

```python
import functools
import math

import jax
import jax.numpy as jnp
from jax import lax
from jax.experimental import pallas as pl
from jax.experimental.pallas import tpu as pltpu
from jax.sharding import PartitionSpec as P

OMEGA = 0.25
GROUP = 32
LANES = 128
MESH = pl.DeviceIdType.MESH

SIN = (4.442882919178189, -7.308245695274183, 3.6063544029247794, -0.8461128632742358, 0.10982698821149484)
COS = (1.4142134964903517, -6.978850985165349, 5.739461140914948, -1.8835629076104397, 0.310698190958135)

f32 = jnp.float32
bf16 = jnp.bfloat16


def horner(coefs, u):
    value = coefs[-1] * u + coefs[-2]
    for c in coefs[-3::-1]:
        value = value * u + c
    return value


def cos_sin(turns):
    r = turns - jnp.round(turns)
    u = r * r
    s = r * horner(SIN, u)
    c = horner(COS, u)
    return 1.0 - s * s, s * c


def iota(shape, dim):
    return lax.broadcasted_iota(jnp.int32, shape, dim)


def nt(a, b):
    return lax.dot_general(a, b, (((1,), (1,)), ((), ())), preferred_element_type=f32)


def nn(a, b):
    return lax.dot_general(a, b, (((1,), (0,)), ((), ())), preferred_element_type=f32)


def split3(x):
    high = x.astype(bf16).astype(f32)
    rest = x - high
    mid = rest.astype(bf16).astype(f32)
    return jnp.concatenate([high, mid, rest - mid], axis=0).astype(bf16)


def joined3(y):
    n = y.shape[0] // 3
    return y[:n] + y[n : 2 * n] + y[2 * n :]


def one_hot(mask):
    return jnp.where(mask, 1.0, 0.0).astype(bf16)


def peer_of(k, o, nd, nt_):
    d = lax.axis_index("depth")
    t = lax.axis_index("track")
    return (lax.rem(d + k, nd), lax.rem(t + o + nt_, nt_))


def near_copies(nd, nt_, src, tile, into, send, recv):
    return [
        pltpu.make_async_remote_copy(
            src.at[pl.ds(tile, 8)],
            into.at[pl.ds(8 * (k - 1), 8)],
            send,
            recv,
            device_id=peer_of(k, 0, nd, nt_),
            device_id_type=MESH,
        )
        for k in range(1, nd)
    ]


def side_copies(nd, nt_, src, tile, into, send, recv):
    depth = src.shape[0]
    copies = []
    for i, o in enumerate((1, -1)):
        copies.append(
            pltpu.make_async_remote_copy(
                src,
                into.at[pl.ds(i * depth, depth)],
                send,
                recv,
                device_id=peer_of(0, o, nd, nt_),
                device_id_type=MESH,
            )
        )
        for k in range(1, nd):
            copies.append(
                pltpu.make_async_remote_copy(
                    src.at[pl.ds(tile, 8)],
                    into.at[pl.ds(2 * depth + 8 * (2 * (k - 1) + i), 8)],
                    send,
                    recv,
                    device_id=peer_of(k, o, nd, nt_),
                    device_id_type=MESH,
                )
            )
    return copies


def wait_all(into, send, recv, nd, nt_):
    copy = pltpu.make_async_remote_copy(
        into, into, send, recv, device_id=peer_of(1, 0, nd, nt_), device_id_type=MESH
    )
    copy.wait_recv()
    copy.wait_send()


WIDE = 256
PER_STEP = 16


def main_kernel(
    nd,
    ntr,
    nchunk,
    slow_hbm,
    cells_hbm,
    taper_hbm,
    secant_hbm,
    prim_hbm,
    quad_hbm,
    seen_hbm,
    grad,
    focused,
    cells,
    taper,
    secant,
    seen,
    slow,
    prim,
    quad,
    weights,
    line,
    spread,
    fint,
    bint,
    fedge,
    blo,
    bhi,
    fside,
    loside,
    hiside,
    edge_of,
    to_own,
    to_lo,
    to_hi,
    halo_a,
    near_a,
    side_a,
    halo_c,
    near_c,
    sides_mine,
    sides,
    side_of,
    phase,
    rot,
    cells_mine,
    cell_rows,
    mine,
    packets,
    below_mine,
    belows,
    ghigh,
    glow,
    block_of,
    place_of,
    rows_of,
    small_sem,
    slow_sem,
    prim_sem,
    quad_sem,
    send_a,
    recv_a,
    send_as,
    recv_as,
    send_cells,
    recv_cells,
    send_s,
    recv_s,
    send_c,
    recv_c,
    send_p,
    recv_p,
    send_q,
    recv_q,
):
    d = lax.axis_index("depth")
    t = lax.axis_index("track")
    depth, traces, angles = prim.shape
    groups = traces // GROUP
    zc = depth // nchunk
    per = LANES // groups

    barrier = pltpu.get_barrier_semaphore()
    slow_copy = pltpu.make_async_copy(slow_hbm, slow, slow_sem)
    small = [
        pltpu.make_async_copy(cells_hbm, cells, small_sem.at[0]),
        pltpu.make_async_copy(taper_hbm, taper, small_sem.at[1]),
        pltpu.make_async_copy(secant_hbm, secant, small_sem.at[2]),
        pltpu.make_async_copy(seen_hbm, seen, small_sem.at[3]),
    ]
    small[0].start()
    slow_copy.start()

    @pl.loop(1, ntr)
    def _(k):
        pl.semaphore_signal(barrier, inc=1, device_id=(d, lax.rem(t + k, ntr)), device_id_type=MESH)

    for k in range(1, nd):
        for o in (-1, 0, 1):
            pl.semaphore_signal(barrier, inc=1, device_id=peer_of(k, o, nd, ntr), device_id_type=MESH)
    for copy in small[1:]:
        copy.start()

    def chunk_copies(i):
        rows = pl.ds(i * zc, zc)
        return (
            pltpu.make_async_copy(prim_hbm.at[rows], prim.at[rows], prim_sem.at[i]),
            pltpu.make_async_copy(quad_hbm.at[rows], quad.at[rows], quad_sem.at[i]),
        )

    mine_lane = iota((depth, LANES), 1)
    zrow = iota((depth, LANES), 0)
    small[0].wait()
    slow_copy.wait()

    @pl.loop(0, nchunk)
    def _(i):
        for copy in chunk_copies(i):
            copy.start()

    own = jnp.zeros((depth, LANES), f32)
    for g in range(groups):
        c = cells[g]
        block = slow[:, lax.div(c, LANES)].reshape(depth, LANES)
        column = jnp.sum(jnp.where(mine_lane == lax.rem(c, LANES), block, 0.0), axis=1, keepdims=True)
        own = jnp.where(mine_lane == g, column, own)
    s = 1
    while s < depth:
        own = own + jnp.where(zrow >= s, pltpu.roll(own, s, 0), 0.0)
        s *= 2
    halo_a[...] = own

    pl.semaphore_wait(barrier, ntr - 1 + 3 * (nd - 1))
    for copy in near_copies(nd, ntr, halo_a, depth - 8, near_a, send_a, recv_a):
        copy.start()
    for copy in side_copies(nd, ntr, halo_a, depth - 8, side_a, send_as, recv_as):
        copy.start()

    lane1 = iota((1, LANES), 1)
    shift = groups * lax.rem(t, per)
    row = jnp.zeros((1, LANES), f32)
    for g in range(groups):
        row = jnp.where(lane1 == shift + g, cells[g].astype(f32), row)
    cells_mine[...] = row
    cell_rows[t] = row

    def to_track(k, src, into, send, recv):
        pltpu.make_async_remote_copy(
            src,
            into.at[t],
            send,
            recv,
            device_id=(d, lax.rem(t + k, ntr)),
            device_id_type=MESH,
        ).start()

    @pl.loop(1, ntr)
    def _(k):
        to_track(k, cells_mine, cell_rows, send_cells, recv_cells)

    def others(ref):
        return ref.at[pl.ds(0, ntr - 1)]

    def track_row(ref, col):
        acc = ref[col * per]
        for j in range(1, per):
            acc = acc + ref[col * per + j]
        return acc

    for copy in small[1:]:
        copy.wait()
    taps = taper[...]
    sec = secant[...] * OMEGA
    row = iota((8, angles), 0)
    nlo = jnp.where(row < 4, 4 - row, 12 - row)
    wlo = jnp.zeros((8, angles), f32)
    whi = jnp.zeros((8, angles), f32)
    for k in range(taper.shape[0]):
        tap = jnp.broadcast_to(taps[k : k + 1, :] * sec, (8, angles))
        wlo = wlo + jnp.where(k < nlo, tap, 0.0)
        whi = whi + jnp.where(k < nlo, 0.0, tap)
    weights[0] = wlo
    weights[1] = whi
    weights[2] = jnp.broadcast_to(jnp.sum(taps, axis=0, keepdims=True) * sec, (8, angles))

    nedge = groups * 8
    e = iota((nedge, traces), 0)
    x = iota((nedge, traces), 1)
    i = lax.rem(e, 8)
    at = lax.rem(lax.div(e, 8) * GROUP + jnp.where(i < 4, i, i - 8) + traces, traces)
    edge_of[...] = one_hot(at == x)
    to_own[...] = one_hot(lax.div(iota((traces, LANES), 0), GROUP) == iota((traces, LANES), 1))
    eb = iota((nedge, LANES), 0)
    el = iota((nedge, LANES), 1)
    bi = lax.div(eb, 8)
    behind_row = lax.rem(eb, 8) < 4
    to_lo[...] = one_hot(jnp.where(bi > 0, bi - 1, jnp.where(behind_row, groups, groups - 1)) == el)
    to_hi[...] = one_hot(jnp.where((bi > 0) | behind_row, bi, groups + 1) == el)
    seen_edge = joined3(nt(split3(seen[...]), edge_of[...]))

    def near_total(into, rowi, up):
        acc = jnp.zeros((1, LANES), f32)
        for k in range(1, nd):
            at = 8 * (k - 1) + rowi
            acc = acc + jnp.where((k <= d) if up else (k > d), into[at : at + 1, :], 0.0)
        return acc

    def side_total(i, rowi, into, up):
        acc = into[i * depth : (i + 1) * depth, :]
        for k in range(1, nd):
            use = (k <= d) if up else (k > d)
            at = 2 * depth + 8 * (2 * (k - 1) + i) + rowi
            acc = acc + jnp.where(use, into[at : at + 1, :], 0.0)
        return acc

    turn = 1.0 / (2.0 * math.pi)
    line[...] = own * turn

    def spread_rows(first, count):
        diagonal = iota((count, LANES), 0) + first == iota((count, LANES), 1)

        @pl.loop(0, depth, unroll=SPREAD_UNROLL)
        def _(z):
            lines = jnp.broadcast_to(line[pl.ds(z, 1), :], (count, LANES))
            spread[z, first : first + count, :] = jnp.broadcast_to(
                jnp.sum(jnp.where(diagonal, lines, 0.0), axis=1, keepdims=True), (count, LANES)
            )

    spread_rows(0, groups)

    sub = iota((8, angles), 0)
    upper = sub < 4
    sub128 = iota((8, LANES), 0)
    lane128 = iota((8, LANES), 1)
    place = lax.rem(lane128, 8) == sub128
    half = 256
    own_group = sub == lax.div(iota((8, half), 1), GROUP)

    def splat(z, r):
        return jnp.broadcast_to(spread[z, r : r + 1, :], (8, LANES))

    def widened(v):
        return jnp.concatenate([v] * (angles // LANES), axis=1)

    nhalf = traces // half

    def local_phases(z):
        for h in range(nhalf):
            c, s = cos_sin(weights[2] * widened(spread[z, 8 * h : 8 * h + 8, :]))
            phase[z, groups + h, 0] = c
            phase[z, groups + h, 1] = s
        for b in range(1, groups):
            c, s = cos_sin(weights[0] * widened(splat(z, b - 1)) + weights[1] * widened(splat(z, b)))
            phase[z, b, 0] = c
            phase[z, b, 1] = s

    def edge_rows(ref, z, b):
        behind = ref[z, GROUP * b : GROUP * b + 8, :].astype(f32)
        stop = GROUP * b if b else traces
        before = ref[z, stop - 8 : stop, :].astype(f32)
        return jnp.where(upper, behind, before)

    def edge_sums(pe, qe, c, s):
        g = qe * c - pe * s
        return [jnp.sum(v, axis=1, keepdims=True) for v in (pe * c + qe * s, g * weights[0], g * weights[1])]

    def inside(z):
        for h in range(nhalf):
            c0 = phase[z, groups + h, 0]
            s0 = phase[z, groups + h, 1]
            ca = rot[groups + h, 0]
            sa = rot[groups + h, 1]
            c = c0 * ca - s0 * sa
            s = s0 * ca + c0 * sa
            w = weights[2]
            wc = w * c
            ws = w * s

            def pair(v):
                return [v, v - v.astype(bf16).astype(f32)]

            lhs_p = jnp.concatenate(pair(c) + pair(-ws), axis=0).astype(bf16)
            lhs_q = jnp.concatenate(pair(s) + pair(wc), axis=0).astype(bf16)
            rows = pl.ds(h * half, half)
            out = nt(lhs_p, prim[z, rows, :]) + nt(lhs_q, quad[z, rows, :])
            fsum = jnp.where(own_group, out[0:8] + out[8:16], 0.0)
            bsum = jnp.where(own_group, out[16:24] + out[24:32], 0.0)
            fint[pl.ds(z, 1), rows] = jnp.sum(fsum, axis=0, keepdims=True)
            bint[pl.ds(z, 1), rows] = jnp.sum(bsum, axis=0, keepdims=True)

    def boundary(zs, b, accs):
        here = lax.div(lane128, 8) == b
        ca = rot[b, 0]
        sa = rot[b, 1]
        out = []
        for z, acc in zip(zs, accs):
            p = edge_rows(prim, z, b)
            q = edge_rows(quad, z, b)
            found = edge_sums(p * ca + q * sa, q * ca - p * sa, phase[z, b, 0], phase[z, b, 1])
            out.append([jnp.where(here, v, a) for v, a in zip(found, acc)])
        return out

    def each_depth(zs):
        accs = [[jnp.zeros((8, LANES), f32)] * 3 for _ in zs]
        every = max(1, (groups - 1) // len(zs))
        for b in range(1, groups):
            if (b - 1) % every == 0 and (b - 1) // every < len(zs):
                inside(zs[(b - 1) // every])
            accs = boundary(zs, b, accs)
        for z, acc in zip(zs, accs):
            for a, ref in zip(acc, (fedge, blo, bhi)):
                ref[pl.ds(z, 1), :] = jnp.sum(jnp.where(place, a, 0.0), axis=0, keepdims=True)

    def outer_edge(z):
        before = jnp.where(sub128 < 4, splat(z, groups), splat(z, groups + 3))
        behind = jnp.where(sub128 < 4, splat(z, groups + 2), splat(z, groups + 1))
        c, s = cos_sin(weights[0] * widened(before) + weights[1] * widened(behind))
        found = edge_sums(edge_rows(prim, z, 0), edge_rows(quad, z, 0), c, s)
        for v, ref in zip(found, (fside, loside, hiside)):
            picked = jnp.where(place & (lane128 < 8), v, 0.0)
            ref[pl.ds(z, 1), :] = jnp.sum(picked, axis=0, keepdims=True)

    @pl.loop(0, depth, unroll=T_UNROLL)
    def _(z):
        local_phases(z)

    wait_all(near_a, send_a, recv_a, nd, ntr)
    above = near_total(near_a, 7, True)
    diagonal = iota((groups, LANES), 0) == iota((groups, LANES), 1)
    lines = jnp.where(diagonal, jnp.broadcast_to(above * turn, (groups, LANES)), 0.0)
    above_rows = jnp.broadcast_to(jnp.sum(lines, axis=1, keepdims=True), (groups, LANES))
    for h in range(nhalf):
        c, s = cos_sin(weights[2] * widened(above_rows[8 * h : 8 * h + 8]))
        rot[groups + h, 0] = c
        rot[groups + h, 1] = s
    for b in range(1, groups):
        lo = jnp.broadcast_to(above_rows[b - 1 : b], (8, LANES))
        hi = jnp.broadcast_to(above_rows[b : b + 1], (8, LANES))
        c, s = cos_sin(weights[0] * widened(lo) + weights[1] * widened(hi))
        rot[b, 0] = c
        rot[b, 1] = s

    @pl.loop(0, nchunk)
    def _(i):
        for copy in chunk_copies(i):
            copy.wait()

        each_depth([i * zc + j for j in range(zc)])

    wait_all(side_a, send_as, recv_as, nd, ntr)
    left = jnp.where(t > 0, side_total(0, 7, side_a, True), 0.0) * turn
    right = jnp.where(t < ntr - 1, side_total(1, 7, side_a, True), 0.0) * turn
    centre = (own + above) * turn
    outer = jnp.where(mine_lane == groups, pltpu.roll(left, 1, 1), 0.0)
    outer = jnp.where(mine_lane == groups + 1, pltpu.roll(right, groups + 1, 1), outer)
    outer = jnp.where(mine_lane == groups + 2, pltpu.roll(centre, groups + 2, 1), outer)
    line[...] = jnp.where(mine_lane == groups + 3, pltpu.roll(centre, 4, 1), outer)
    spread_rows(groups, 8)

    @pl.loop(0, depth, unroll=OUTER_UNROLL)
    def _(z):
        outer_edge(z)

    def suffix(v):
        s = 1
        while s < depth:
            v = v + jnp.where(zrow < depth - s, pltpu.roll(v, depth - s, 0), 0.0)
            s *= 2
        return v

    xoff = lax.rem(iota((depth, traces), 1), GROUP)
    inner = (xoff >= 4) & (xoff < GROUP - 4)
    term = jnp.where(inner, (fint[...] - seen[...]) * bint[...], 0.0)
    edge = fedge[...] + fside[...]
    resid = edge - seen_edge
    sums = joined3(nn(split3(term), to_own[...]))
    sums = sums + joined3(nn(split3(resid * (blo[...] + loside[...])), to_lo[...]))
    sums = sums + joined3(nn(split3(resid * (bhi[...] + hiside[...])), to_hi[...]))
    sums = jnp.where((t == 0) & (mine_lane == groups), 0.0, sums)
    sums = jnp.where((t == ntr - 1) & (mine_lane == groups + 1), 0.0, sums)
    sums = suffix(sums)
    halo_c[...] = sums
    for copy in near_copies(nd, ntr, halo_c, 0, near_c, send_c, recv_c):
        copy.start()

    grads = jnp.where(mine_lane < groups, sums, 0.0)
    packet = jnp.zeros((8, LANES), f32)
    for q in range(depth // 8):
        block = grads[8 * q : 8 * q + 8]
        packet = packet + (pltpu.roll(block, groups * q, 1) if q else block)
    packet = packet + pltpu.roll(pltpu.roll(packet, 4, 0), LANES // 2, 1)
    packet = pltpu.roll(packet, shift, 1)[0:4]
    mine[...] = packet
    packets[t] = packet

    @pl.loop(1, ntr)
    def _(k):
        to_track(k, mine, packets, send_p, recv_p)

    before = jnp.sum(jnp.where(mine_lane == groups, sums, 0.0), axis=1, keepdims=True)
    behind = jnp.sum(jnp.where(mine_lane == groups + 1, sums, 0.0), axis=1, keepdims=True)
    row = jnp.where(mine_lane == zrow, before, jnp.where(mine_lane == zrow + depth, behind, 0.0))
    row = jnp.sum(row, axis=0, keepdims=True)
    sides_mine[...] = row
    sides[t] = row

    @pl.loop(1, ntr)
    def _(k):
        to_track(k, sides_mine, sides, send_s, recv_s)

    wait_all(others(cell_rows), send_cells, recv_cells, nd, ntr)
    for col in range(ntr // per):
        lanes = pl.ds(col * LANES, LANES)
        cell = track_row(cell_rows, col)
        block = jnp.floor(cell * (1.0 / WIDE))
        block_of[:, lanes] = jnp.broadcast_to(block, (depth, LANES)).astype(bf16)
        place_of[:, lanes] = one_hot(iota((WIDE, LANES), 0).astype(f32) == cell - block * WIDE)

    srow = iota((LANES, ntr * groups), 0)
    scol = iota((LANES, ntr * groups), 1)
    starget = jnp.where(srow < ntr, srow * groups - 1, (srow - ntr) * groups + groups)
    side_of[...] = one_hot((srow < 2 * ntr) & (starget == scol))

    wait_all(near_c, send_c, recv_c, nd, ntr)
    total_row = jnp.broadcast_to(near_total(near_c, 0, False), (8, LANES))
    below = pltpu.roll(jnp.where(lane128 < groups, total_row, 0.0), shift, 1)
    before = pltpu.roll(jnp.where(lane128 == groups, total_row, 0.0), lax.rem(t + LANES - groups, LANES), 1)
    behind = pltpu.roll(jnp.where(lane128 == groups + 1, total_row, 0.0), lax.rem(t + LANES + ntr - groups - 1, LANES), 1)
    below = jnp.where(sub128 == 0, below, before + behind)[0:2]
    below_mine[...] = below
    belows[t] = below

    @pl.loop(1, ntr)
    def _(k):
        to_track(k, below_mine, belows, send_q, recv_q)

    focused[...] = jnp.where(inner, fint[...], joined3(nn(split3(edge), edge_of[...])))
    wait_all(others(packets), send_p, recv_p, nd, ntr)

    wait_all(others(sides), send_s, recv_s, nd, ntr)
    blocks = []
    for j in range(ntr // 8):
        acc = jnp.zeros((8, LANES), f32)
        for i in range(8):
            acc = jnp.where(sub128 == i, jnp.broadcast_to(sides[8 * j + i], (8, LANES)), acc)
        blocks.append(acc)
    turned = jnp.concatenate(blocks, axis=0).T
    turned = jnp.concatenate([turned[0:depth], turned[depth : 2 * depth]], axis=1)
    side_terms = joined3(nn(split3(turned), side_of[0 : 2 * ntr, :]))
    chunk = lax.div(iota((4, LANES), 1), groups)
    for col in range(ntr // per):
        parts = []
        for c in range(per):
            acc = jnp.zeros((4, LANES), f32)
            for j in range(per):
                acc = jnp.where(chunk == (c + j) % per, packets[col * per + j], acc)
            parts.append(acc)
        lanes = pl.ds(col * LANES, LANES)
        nq = depth // 8
        pieces = []
        for q in range(nq):
            for h in range(2):
                c = q + nq * h
                both = jnp.concatenate([parts[c], parts[c]], axis=0)
                pieces.append(pltpu.roll(both, LANES - groups * c, 1) if c else both)
        low_rows = iota((8, LANES), 0) < 4
        g = jnp.concatenate(
            [jnp.where(low_rows, pieces[2 * q], pieces[2 * q + 1]) for q in range(nq)], axis=0
        )
        g = g + side_terms[:, col * LANES : (col + 1) * LANES]
        high = g.astype(bf16)
        ghigh[:, lanes] = high
        glow[:, lanes] = (g - high.astype(f32)).astype(bf16)

    nblock = grad.shape[1] // WIDE

    @pl.loop(0, nblock // PER_STEP)
    def _(step):
        highs = []
        lows = []
        for j in range(PER_STEP):
            mask = block_of[...] == (step * PER_STEP + j).astype(bf16)
            highs.append(jnp.where(mask, ghigh[...], jnp.zeros((), bf16)))
            lows.append(jnp.where(mask, glow[...], jnp.zeros((), bf16)))
        out = nt(jnp.concatenate(highs, axis=0), place_of[...]) + nt(jnp.concatenate(lows, axis=0), place_of[...])
        out = jnp.concatenate([out[depth * j : depth * (j + 1)] for j in range(PER_STEP)], axis=1)
        wide = PER_STEP * WIDE
        grad[:, pl.ds(pl.multiple_of(step * wide, wide), wide)] = out

    wait_all(others(belows), send_q, recv_q, nd, ntr)
    tops = [track_row(belows, col) for col in range(ntr // per)]
    extra = tops[0]
    for top in tops[1:]:
        extra = extra + top
    extra = jnp.broadcast_to(extra[1:2], (8, LANES))
    below = jnp.concatenate([top[0:1] for top in tops], axis=1) + joined3(nn(split3(extra), side_of[...]))[0:1]
    below = jnp.broadcast_to(below, (nblock, ntr * groups))
    blocks = jnp.broadcast_to(block_of[...].astype(f32)[0:1], (nblock, ntr * groups))
    spread_below = jnp.where(blocks == iota((nblock, ntr * groups), 0).astype(f32), below, 0.0)
    rows_of[...] = joined3(nt(split3(spread_below), place_of[...]))

    @pl.loop(0, nblock, unroll=8)
    def _(j):
        lanes = pl.ds(pl.multiple_of(j * WIDE, WIDE), WIDE)
        grad[:, lanes] = grad[:, lanes] + jnp.broadcast_to(rows_of[pl.ds(j, 1), :], (depth, WIDE))


T_UNROLL = 4
SPREAD_UNROLL = 32
OUTER_UNROLL = 32
OUT_PARTS = 1
AT_ONCE = 8


def on_device(nd, ntr, slowness_cells, cell_of_group, taper, secant, primary, quadrature, observed):
    depth, traces, angles = primary.shape
    taps = taper.shape[1]
    ncell = slowness_cells.shape[1]
    groups = cell_of_group.shape[0]
    nedge = groups * 8
    total = ntr * groups
    nchunk = depth // AT_ONCE
    vmem = pl.BlockSpec(memory_space=pltpu.VMEM)
    anywhere = pl.BlockSpec(memory_space=pl.ANY)
    near = nd - 1
    dma = pltpu.SemaphoreType.DMA
    V = pltpu.VMEM
    slow = slowness_cells.reshape(depth // 8, 8, ncell // LANES, LANES).transpose(0, 2, 1, 3)
    gradient, image = pl.pallas_call(
        functools.partial(main_kernel, nd, ntr, nchunk),
        out_shape=(
            jax.ShapeDtypeStruct((depth, ncell), f32),
            jax.ShapeDtypeStruct((depth, traces), f32),
        ),
        in_specs=[anywhere] * 7,
        out_specs=(vmem, vmem),
        scratch_shapes=[
            pltpu.SMEM((groups,), jnp.int32),
            V((taps, angles), f32),
            V((1, angles), f32),
            V((depth, traces), f32),
            V(slow.shape, f32),
            V((depth, traces, angles), bf16),
            V((depth, traces, angles), bf16),
            V((3, 8, angles), f32),
            V((depth, LANES), f32),
            V((depth, 24, LANES), f32),
            V((depth, traces), f32),
            V((depth, traces), f32),
        ]
        + [V((depth, nedge), f32)] * 6
        + [
            V((nedge, traces), bf16),
            V((traces, LANES), bf16),
            V((nedge, LANES), bf16),
            V((nedge, LANES), bf16),
            V((depth, LANES), f32),
            V((8 * near, LANES), f32),
            V((2 * depth + 16 * near, LANES), f32),
            V((depth, LANES), f32),
            V((8 * near, LANES), f32),
            V((1, LANES), f32),
            V((ntr, 1, LANES), f32),
            V((LANES, total), bf16),
            V((depth, groups + traces // 256, 2, 8, angles), f32),
            V((groups + traces // 256, 2, 8, angles), f32),
            V((1, LANES), f32),
            V((ntr, 1, LANES), f32),
            V((4, LANES), f32),
            V((ntr, 4, LANES), f32),
            V((2, LANES), f32),
            V((ntr, 2, LANES), f32),
            V((depth, total), bf16),
            V((depth, total), bf16),
            V((depth, total), bf16),
            V((WIDE, total), bf16),
            V((ncell // WIDE, WIDE), f32),
            dma((4,)),
            dma,
            dma((nchunk,)),
            dma((nchunk,)),
        ]
        + [dma] * 14,
        compiler_params=pltpu.CompilerParams(
            collective_id=0,
            has_side_effects=True,
            vmem_limit_bytes=VMEM_LIMIT,
        ),
        name="radargram",
    )(
        *[
            pltpu.with_memory_space_constraint(v, pltpu.HBM)
            for v in (slow, cell_of_group, taper.T, secant.reshape(1, angles), primary, quadrature, observed)
        ]
    )
    gradient, image = pl.pallas_call(
        hand_out,
        out_shape=(
            jax.ShapeDtypeStruct((depth, ncell), f32),
            jax.ShapeDtypeStruct((depth, traces), f32),
        ),
        in_specs=[anywhere] * 2,
        out_specs=(anywhere, anywhere),
        scratch_shapes=[dma((OUT_PARTS + 1,))],
        compiler_params=pltpu.CompilerParams(vmem_limit_bytes=1024 * 1024),
        name="hand_out",
    )(gradient, image)
    return image, gradient


def hand_out(grad, image, grad_out, image_out, sems):
    rows = grad.shape[0] // OUT_PARTS
    copies = [pltpu.make_async_copy(image, image_out, sems.at[OUT_PARTS])]
    for i in range(OUT_PARTS):
        part = pl.ds(i * rows, rows)
        copies.append(pltpu.make_async_copy(grad.at[part], grad_out.at[part], sems.at[i]))
    for copy in copies:
        copy.start()
    for copy in copies:
        copy.wait()


VMEM_LIMIT = 40 * 1024 * 1024


def solution(mesh):
    in_specs = (
        P("depth", None),
        P("track"),
        P(),
        P(),
        P("depth", "track", None),
        P("depth", "track", None),
        P("depth", "track"),
    )
    out_specs = (P("depth", "track"), P("depth", None))
    nd = mesh.shape["depth"]
    ntr = mesh.shape["track"]
    return jax.shard_map(
        functools.partial(on_device, nd, ntr), mesh=mesh, in_specs=in_specs, out_specs=out_specs, check_vma=False
    )
```

```python
import functools
import math

import jax
import jax.numpy as jnp
from jax import lax
from jax.experimental import pallas as pl
from jax.experimental.pallas import tpu as pltpu
from jax.sharding import PartitionSpec as P

OMEGA = 0.25
GROUP = 32
LANES = 128
MESH = pl.DeviceIdType.MESH

SIN = (4.442882919178189, -7.308245695274183, 3.6063544029247794, -0.8461128632742358, 0.10982698821149484)
COS = (1.4142134964903517, -6.978850985165349, 5.739461140914948, -1.8835629076104397, 0.310698190958135)

f32 = jnp.float32
bf16 = jnp.bfloat16


def horner(coefs, u):
    value = coefs[-1] * u + coefs[-2]
    for c in coefs[-3::-1]:
        value = value * u + c
    return value


def cos_sin(turns):
    r = turns - jnp.round(turns)
    u = r * r
    s = r * horner(SIN, u)
    c = horner(COS, u)
    return 1.0 - s * s, s * c


def iota(shape, dim):
    return lax.broadcasted_iota(jnp.int32, shape, dim)


def part(x, n):
    return lax.shift_right_logical(x, n.bit_length() - 1)


def inside_part(x, n):
    return x & (n - 1)


def nt(a, b):
    return lax.dot_general(a, b, (((1,), (1,)), ((), ())), preferred_element_type=f32)


def nn(a, b):
    return lax.dot_general(a, b, (((1,), (0,)), ((), ())), preferred_element_type=f32)


def split3(x):
    high = x.astype(bf16).astype(f32)
    rest = x - high
    mid = rest.astype(bf16).astype(f32)
    return jnp.concatenate([high, mid, rest - mid], axis=0).astype(bf16)


def joined3(y):
    n = y.shape[0] // 3
    return y[:n] + y[n : 2 * n] + y[2 * n :]


def one_hot(mask):
    return jnp.where(mask, 1.0, 0.0).astype(bf16)


def peer_of(k, o, nd, nt_):
    d = lax.axis_index("depth")
    t = lax.axis_index("track")
    return (lax.rem(d + k, nd), lax.rem(t + o + nt_, nt_))


def near_copies(nd, nt_, src, tile, into, send, recv):
    return [
        pltpu.make_async_remote_copy(
            src.at[pl.ds(tile, 8)],
            into.at[pl.ds(8 * (k - 1), 8)],
            send,
            recv,
            device_id=peer_of(k, 0, nd, nt_),
            device_id_type=MESH,
        )
        for k in range(1, nd)
    ]


def side_copies(nd, nt_, src, tile, into, send, recv):
    depth = src.shape[0]
    copies = []
    for i, o in enumerate((1, -1)):
        copies.append(
            pltpu.make_async_remote_copy(
                src,
                into.at[pl.ds(i * depth, depth)],
                send,
                recv,
                device_id=peer_of(0, o, nd, nt_),
                device_id_type=MESH,
            )
        )
        for k in range(1, nd):
            copies.append(
                pltpu.make_async_remote_copy(
                    src.at[pl.ds(tile, 8)],
                    into.at[pl.ds(2 * depth + 8 * (2 * (k - 1) + i), 8)],
                    send,
                    recv,
                    device_id=peer_of(k, o, nd, nt_),
                    device_id_type=MESH,
                )
            )
    return copies


def wait_all(into, send, recv, nd, nt_):
    copy = pltpu.make_async_remote_copy(
        into, into, send, recv, device_id=peer_of(1, 0, nd, nt_), device_id_type=MESH
    )
    copy.wait_recv()
    copy.wait_send()


WIDE = 256
PER_STEP = 16


def main_kernel(
    nd,
    ntr,
    nchunk,
    slow_hbm,
    cells_hbm,
    taper_hbm,
    secant_hbm,
    prim_hbm,
    quad_hbm,
    seen_hbm,
    grad,
    focused,
    cells,
    taper,
    secant,
    seen,
    slow,
    prim,
    quad,
    weights,
    line,
    spread,
    fint,
    bint,
    fedge,
    blo,
    bhi,
    fside,
    loside,
    hiside,
    edge_of,
    to_own,
    to_lo,
    to_hi,
    halo_a,
    near_a,
    side_a,
    below_sum,
    sides_mine,
    sides,
    side_of,
    phase,
    rot,
    cells_mine,
    cell_rows,
    mine,
    packets,
    below_mine,
    belows,
    ghigh,
    glow,
    block_of,
    place_of,
    rows_of,
    small_sem,
    slow_sem,
    prim_sem,
    quad_sem,
    send_a,
    recv_a,
    send_as,
    recv_as,
    send_cells,
    recv_cells,
    send_s,
    recv_s,
    send_p,
    recv_p,
    send_q,
    recv_q,
):
    d = lax.axis_index("depth")
    t = lax.axis_index("track")
    depth, traces, angles = prim.shape
    groups = traces // GROUP
    zc = depth // nchunk
    per = LANES // groups

    barrier = pltpu.get_barrier_semaphore()
    slow_copy = pltpu.make_async_copy(slow_hbm, slow, slow_sem)
    small = [
        pltpu.make_async_copy(cells_hbm, cells, small_sem.at[0]),
        pltpu.make_async_copy(taper_hbm, taper, small_sem.at[1]),
        pltpu.make_async_copy(secant_hbm, secant, small_sem.at[2]),
        pltpu.make_async_copy(seen_hbm, seen, small_sem.at[3]),
    ]
    small[0].start()
    slow_copy.start()

    @pl.loop(1, ntr)
    def _(k):
        pl.semaphore_signal(barrier, inc=1, device_id=(d, lax.rem(t + k, ntr)), device_id_type=MESH)

    for k in range(1, nd):
        for o in (-1, 0, 1):
            pl.semaphore_signal(barrier, inc=1, device_id=peer_of(k, o, nd, ntr), device_id_type=MESH)
    for copy in small[1:]:
        copy.start()

    def chunk_copies(i):
        rows = pl.ds(i * zc, zc)
        return (
            pltpu.make_async_copy(prim_hbm.at[rows], prim.at[rows], prim_sem.at[i]),
            pltpu.make_async_copy(quad_hbm.at[rows], quad.at[rows], quad_sem.at[i]),
        )

    mine_lane = iota((depth, LANES), 1)
    zrow = iota((depth, LANES), 0)
    small[0].wait()
    slow_copy.wait()

    @pl.loop(0, nchunk)
    def _(i):
        for copy in chunk_copies(i):
            copy.start()

    own = jnp.zeros((depth, LANES), f32)
    for g in range(groups):
        c = cells[g]
        block = slow[:, lax.div(c, LANES)].reshape(depth, LANES)
        column = jnp.sum(jnp.where(mine_lane == lax.rem(c, LANES), block, 0.0), axis=1, keepdims=True)
        own = jnp.where(mine_lane == g, column, own)
    s = 1
    while s < depth:
        own = own + jnp.where(zrow >= s, pltpu.roll(own, s, 0), 0.0)
        s *= 2
    halo_a[...] = own

    pl.semaphore_wait(barrier, ntr - 1 + 3 * (nd - 1))
    for copy in near_copies(nd, ntr, halo_a, depth - 8, near_a, send_a, recv_a):
        copy.start()
    for copy in side_copies(nd, ntr, halo_a, depth - 8, side_a, send_as, recv_as):
        copy.start()

    lane1 = iota((1, LANES), 1)
    shift = groups * lax.rem(t, per)
    row = jnp.zeros((1, LANES), f32)
    for g in range(groups):
        row = jnp.where(lane1 == shift + g, cells[g].astype(f32), row)
    cells_mine[...] = row
    cell_rows[t] = row

    def to_track(k, src, into, send, recv):
        pltpu.make_async_remote_copy(
            src,
            into.at[t],
            send,
            recv,
            device_id=(d, lax.rem(t + k, ntr)),
            device_id_type=MESH,
        ).start()

    @pl.loop(1, ntr)
    def _(k):
        to_track(k, cells_mine, cell_rows, send_cells, recv_cells)

    def others(ref):
        return ref.at[pl.ds(0, ntr - 1)]

    def track_row(ref, col):
        acc = ref[col * per]
        for j in range(1, per):
            acc = acc + ref[col * per + j]
        return acc

    for copy in small[1:]:
        copy.wait()
    taps = taper[...]
    sec = secant[...] * OMEGA
    row = iota((8, angles), 0)
    nlo = jnp.where(row < 4, 4 - row, 12 - row)
    wlo = jnp.zeros((8, angles), f32)
    whi = jnp.zeros((8, angles), f32)
    for k in range(taper.shape[0]):
        tap = jnp.broadcast_to(taps[k : k + 1, :] * sec, (8, angles))
        wlo = wlo + jnp.where(k < nlo, tap, 0.0)
        whi = whi + jnp.where(k < nlo, 0.0, tap)
    weights[0] = wlo
    weights[1] = whi
    weights[2] = jnp.broadcast_to(jnp.sum(taps, axis=0, keepdims=True) * sec, (8, angles))

    nedge = groups * 8
    e = iota((nedge, traces), 0)
    x = iota((nedge, traces), 1)
    i = inside_part(e, 8)
    at = inside_part(part(e, 8) * GROUP + jnp.where(i < 4, i, i - 8) + traces, traces)
    edge_of[...] = one_hot(at == x)
    to_own[...] = one_hot(part(iota((traces, LANES), 0), GROUP) == iota((traces, LANES), 1))
    eb = iota((nedge, LANES), 0)
    el = iota((nedge, LANES), 1)
    bi = part(eb, 8)
    behind_row = inside_part(eb, 8) < 4
    to_lo[...] = one_hot(jnp.where(bi > 0, bi - 1, jnp.where(behind_row, groups, groups - 1)) == el)
    to_hi[...] = one_hot(jnp.where((bi > 0) | behind_row, bi, groups + 1) == el)
    seen_edge = joined3(nt(split3(seen[...]), edge_of[...]))

    def near_total(into, rowi, up):
        acc = jnp.zeros((1, LANES), f32)
        for k in range(1, nd):
            at = 8 * (k - 1) + rowi
            acc = acc + jnp.where((k <= d) if up else (k > d), into[at : at + 1, :], 0.0)
        return acc

    def side_total(i, rowi, into, up):
        acc = into[i * depth : (i + 1) * depth, :]
        for k in range(1, nd):
            use = (k <= d) if up else (k > d)
            at = 2 * depth + 8 * (2 * (k - 1) + i) + rowi
            acc = acc + jnp.where(use, into[at : at + 1, :], 0.0)
        return acc

    turn = 1.0 / (2.0 * math.pi)
    line[...] = own * turn

    def spread_rows(first, count):
        diagonal = iota((count, LANES), 0) + first == iota((count, LANES), 1)

        @pl.loop(0, depth, unroll=SPREAD_UNROLL)
        def _(z):
            lines = jnp.broadcast_to(line[pl.ds(z, 1), :], (count, LANES))
            spread[z, first : first + count, :] = jnp.broadcast_to(
                jnp.sum(jnp.where(diagonal, lines, 0.0), axis=1, keepdims=True), (count, LANES)
            )

    spread_rows(0, groups)

    sub = iota((8, angles), 0)
    upper = sub < 4
    sub128 = iota((8, LANES), 0)
    lane128 = iota((8, LANES), 1)
    place = inside_part(lane128, 8) == sub128
    half = 256
    own_group = sub == part(iota((8, half), 1), GROUP)

    def splat(z, r):
        return jnp.broadcast_to(spread[z, r : r + 1, :], (8, LANES))

    def widened(v):
        return jnp.concatenate([v] * (angles // LANES), axis=1)

    nhalf = traces // half

    def local_phases(z):
        for h in range(nhalf):
            c, s = cos_sin(weights[2] * widened(spread[z, 8 * h : 8 * h + 8, :]))
            phase[z, groups + h, 0] = c
            phase[z, groups + h, 1] = s
        for b in range(1, groups):
            c, s = cos_sin(weights[0] * widened(splat(z, b - 1)) + weights[1] * widened(splat(z, b)))
            phase[z, b, 0] = c
            phase[z, b, 1] = s

    def edge_rows(ref, z, b):
        behind = ref[z, GROUP * b : GROUP * b + 8, :].astype(f32)
        stop = GROUP * b if b else traces
        before = ref[z, stop - 8 : stop, :].astype(f32)
        return jnp.where(upper, behind, before)

    def edge_sums(pe, qe, c, s):
        g = qe * c - pe * s
        return [jnp.sum(v, axis=1, keepdims=True) for v in (pe * c + qe * s, g * weights[0], g * weights[1])]

    def inside(z):
        for h in range(nhalf):
            c0 = phase[z, groups + h, 0]
            s0 = phase[z, groups + h, 1]
            ca = rot[groups + h, 0]
            sa = rot[groups + h, 1]
            c = c0 * ca - s0 * sa
            s = s0 * ca + c0 * sa
            w = weights[2]
            wc = w * c
            ws = w * s

            def pair(v):
                return [v, v - v.astype(bf16).astype(f32)]

            lhs_p = jnp.concatenate(pair(c) + pair(-ws), axis=0).astype(bf16)
            lhs_q = jnp.concatenate(pair(s) + pair(wc), axis=0).astype(bf16)
            rows = pl.ds(h * half, half)
            out = nt(lhs_p, prim[z, rows, :]) + nt(lhs_q, quad[z, rows, :])
            fsum = jnp.where(own_group, out[0:8] + out[8:16], 0.0)
            bsum = jnp.where(own_group, out[16:24] + out[24:32], 0.0)
            fint[pl.ds(z, 1), rows] = jnp.sum(fsum, axis=0, keepdims=True)
            bint[pl.ds(z, 1), rows] = jnp.sum(bsum, axis=0, keepdims=True)

    def boundary(zs, b, accs):
        here = part(lane128, 8) == b
        ca = rot[b, 0]
        sa = rot[b, 1]
        out = []
        for z, acc in zip(zs, accs):
            p = edge_rows(prim, z, b)
            q = edge_rows(quad, z, b)
            found = edge_sums(p * ca + q * sa, q * ca - p * sa, phase[z, b, 0], phase[z, b, 1])
            out.append([jnp.where(here, v, a) for v, a in zip(found, acc)])
        return out

    def each_depth(zs):
        accs = [[jnp.zeros((8, LANES), f32)] * 3 for _ in zs]
        every = max(1, (groups - 1) // len(zs))
        for b in range(1, groups):
            if (b - 1) % every == 0 and (b - 1) // every < len(zs):
                inside(zs[(b - 1) // every])
            accs = boundary(zs, b, accs)
        for z, acc in zip(zs, accs):
            for a, ref in zip(acc, (fedge, blo, bhi)):
                ref[pl.ds(z, 1), :] = jnp.sum(jnp.where(place, a, 0.0), axis=0, keepdims=True)

    def outer_edge(z):
        before = jnp.where(sub128 < 4, splat(z, groups), splat(z, groups + 3))
        behind = jnp.where(sub128 < 4, splat(z, groups + 2), splat(z, groups + 1))
        c, s = cos_sin(weights[0] * widened(before) + weights[1] * widened(behind))
        found = edge_sums(edge_rows(prim, z, 0), edge_rows(quad, z, 0), c, s)
        for v, ref in zip(found, (fside, loside, hiside)):
            picked = jnp.where(place & (lane128 < 8), v, 0.0)
            ref[pl.ds(z, 1), :] = jnp.sum(picked, axis=0, keepdims=True)

    @pl.loop(0, depth, unroll=T_UNROLL)
    def _(z):
        local_phases(z)

    wait_all(near_a, send_a, recv_a, nd, ntr)
    above = near_total(near_a, 7, True)
    diagonal = iota((groups, LANES), 0) == iota((groups, LANES), 1)
    lines = jnp.where(diagonal, jnp.broadcast_to(above * turn, (groups, LANES)), 0.0)
    above_rows = jnp.broadcast_to(jnp.sum(lines, axis=1, keepdims=True), (groups, LANES))
    for h in range(nhalf):
        c, s = cos_sin(weights[2] * widened(above_rows[8 * h : 8 * h + 8]))
        rot[groups + h, 0] = c
        rot[groups + h, 1] = s
    for b in range(1, groups):
        lo = jnp.broadcast_to(above_rows[b - 1 : b], (8, LANES))
        hi = jnp.broadcast_to(above_rows[b : b + 1], (8, LANES))
        c, s = cos_sin(weights[0] * widened(lo) + weights[1] * widened(hi))
        rot[b, 0] = c
        rot[b, 1] = s

    @pl.loop(0, nchunk)
    def _(i):
        for copy in chunk_copies(i):
            copy.wait()

        each_depth([i * zc + j for j in range(zc)])

    wait_all(side_a, send_as, recv_as, nd, ntr)
    left = jnp.where(t > 0, side_total(0, 7, side_a, True), 0.0) * turn
    right = jnp.where(t < ntr - 1, side_total(1, 7, side_a, True), 0.0) * turn
    centre = (own + above) * turn
    outer = jnp.where(mine_lane == groups, pltpu.roll(left, 1, 1), 0.0)
    outer = jnp.where(mine_lane == groups + 1, pltpu.roll(right, groups + 1, 1), outer)
    outer = jnp.where(mine_lane == groups + 2, pltpu.roll(centre, groups + 2, 1), outer)
    line[...] = jnp.where(mine_lane == groups + 3, pltpu.roll(centre, 4, 1), outer)
    spread_rows(groups, 8)

    @pl.loop(0, depth, unroll=OUTER_UNROLL)
    def _(z):
        outer_edge(z)

    def suffix(v):
        s = 1
        while s < depth:
            v = v + jnp.where(zrow < depth - s, pltpu.roll(v, depth - s, 0), 0.0)
            s *= 2
        return v

    xoff = inside_part(iota((depth, traces), 1), GROUP)
    inner = (xoff >= 4) & (xoff < GROUP - 4)
    term = jnp.where(inner, (fint[...] - seen[...]) * bint[...], 0.0)
    edge = fedge[...] + fside[...]
    resid = edge - seen_edge
    sums = joined3(nn(split3(term), to_own[...]))
    sums = sums + joined3(nn(split3(resid * (blo[...] + loside[...])), to_lo[...]))
    sums = sums + joined3(nn(split3(resid * (bhi[...] + hiside[...])), to_hi[...]))
    sums = jnp.where((t == 0) & (mine_lane == groups), 0.0, sums)
    sums = jnp.where((t == ntr - 1) & (mine_lane == groups + 1), 0.0, sums)
    sums = suffix(sums)

    total_row = jnp.broadcast_to(sums[0:1], (8, LANES))
    below = pltpu.roll(jnp.where(lane128 < groups, total_row, 0.0), shift, 1)
    before = pltpu.roll(jnp.where(lane128 == groups, total_row, 0.0), lax.rem(t + LANES - groups, LANES), 1)
    behind = pltpu.roll(
        jnp.where(lane128 == groups + 1, total_row, 0.0), lax.rem(t + LANES + ntr - groups - 1, LANES), 1
    )
    below_mine[...] = jnp.where(sub128 == 0, below, before + behind)[0:2]

    def above_copy(k, o):
        return pltpu.make_async_remote_copy(
            below_mine,
            belows.at[k - 1, t],
            send_q.at[k - 1],
            recv_q.at[k - 1],
            device_id=(lax.rem(d + nd - k, nd), lax.rem(t + o, ntr)),
            device_id_type=MESH,
        )

    for k in range(nd - 1, 0, -1):

        @pl.when(d >= k)
        def _():
            @pl.loop(0, ntr)
            def _(o):
                above_copy(k, lax.rem(o + ntr // 2, ntr)).start()

    grads = jnp.where(mine_lane < groups, sums, 0.0)
    packet = jnp.zeros((8, LANES), f32)
    for q in range(depth // 8):
        block = grads[8 * q : 8 * q + 8]
        packet = packet + (pltpu.roll(block, groups * q, 1) if q else block)
    packet = packet + pltpu.roll(pltpu.roll(packet, 4, 0), LANES // 2, 1)
    packet = pltpu.roll(packet, shift, 1)[0:4]
    mine[...] = packet
    packets[t] = packet

    @pl.loop(1, ntr)
    def _(k):
        to_track(k, mine, packets, send_p, recv_p)

    before = jnp.sum(jnp.where(mine_lane == groups, sums, 0.0), axis=1, keepdims=True)
    behind = jnp.sum(jnp.where(mine_lane == groups + 1, sums, 0.0), axis=1, keepdims=True)
    row = jnp.where(mine_lane == zrow, before, jnp.where(mine_lane == zrow + depth, behind, 0.0))
    row = jnp.sum(row, axis=0, keepdims=True)
    sides_mine[...] = row
    sides[t] = row

    @pl.loop(1, ntr)
    def _(k):
        to_track(k, sides_mine, sides, send_s, recv_s)

    wait_all(others(cell_rows), send_cells, recv_cells, nd, ntr)
    for col in range(ntr // per):
        lanes = pl.ds(col * LANES, LANES)
        cell = track_row(cell_rows, col)
        block = jnp.floor(cell * (1.0 / WIDE))
        block_of[:, lanes] = jnp.broadcast_to(block, (depth, LANES)).astype(bf16)
        column = jnp.broadcast_to(cell - block * WIDE, (LANES, LANES)).T
        column = jnp.concatenate([column] * (WIDE // LANES), axis=1)
        place_of[lanes, :] = one_hot(iota((LANES, WIDE), 1).astype(f32) == column)

    srow = iota((LANES, ntr * groups), 0)
    scol = iota((LANES, ntr * groups), 1)
    starget = jnp.where(srow < ntr, srow * groups - 1, (srow - ntr) * groups + groups)
    side_of[...] = one_hot((srow < 2 * ntr) & (starget == scol))

    focused[...] = jnp.where(inner, fint[...], joined3(nn(split3(edge), edge_of[...])))
    wait_all(others(packets), send_p, recv_p, nd, ntr)

    wait_all(others(sides), send_s, recv_s, nd, ntr)
    blocks = []
    for j in range(ntr // 8):
        acc = jnp.zeros((8, LANES), f32)
        for i in range(8):
            acc = jnp.where(sub128 == i, jnp.broadcast_to(sides[8 * j + i], (8, LANES)), acc)
        blocks.append(acc)
    turned = jnp.concatenate(blocks, axis=0).T
    turned = jnp.concatenate([turned[0:depth], turned[depth : 2 * depth]], axis=1)
    side_terms = joined3(nn(split3(turned), side_of[0 : 2 * ntr, :]))
    chunk = part(iota((4, LANES), 1), groups)
    for col in range(ntr // per):
        parts = []
        for c in range(per):
            acc = jnp.zeros((4, LANES), f32)
            for j in range(per):
                acc = jnp.where(chunk == (c + j) % per, packets[col * per + j], acc)
            parts.append(acc)
        lanes = pl.ds(col * LANES, LANES)
        nq = depth // 8
        pieces = []
        for q in range(nq):
            for h in range(2):
                c = q + nq * h
                both = jnp.concatenate([parts[c], parts[c]], axis=0)
                pieces.append(pltpu.roll(both, LANES - groups * c, 1) if c else both)
        low_rows = iota((8, LANES), 0) < 4
        g = jnp.concatenate(
            [jnp.where(low_rows, pieces[2 * q], pieces[2 * q + 1]) for q in range(nq)], axis=0
        )
        g = g + side_terms[:, col * LANES : (col + 1) * LANES]
        high = g.astype(bf16)
        ghigh[:, lanes] = high
        glow[:, lanes] = (g - high.astype(f32)).astype(bf16)

    nblock = grad.shape[1] // WIDE

    @pl.loop(0, nblock // PER_STEP)
    def _(step):
        highs = []
        lows = []
        for j in range(PER_STEP):
            mask = block_of[...] == (step * PER_STEP + j).astype(bf16)
            highs.append(jnp.where(mask, ghigh[...], jnp.zeros((), bf16)))
            lows.append(jnp.where(mask, glow[...], jnp.zeros((), bf16)))
        out = nn(jnp.concatenate(highs, axis=0), place_of[...]) + nn(jnp.concatenate(lows, axis=0), place_of[...])
        out = jnp.concatenate([out[depth * j : depth * (j + 1)] for j in range(PER_STEP)], axis=1)
        wide = PER_STEP * WIDE
        grad[:, pl.ds(pl.multiple_of(step * wide, wide), wide)] = out

    below_sum[...] = jnp.zeros(below_sum.shape, f32)
    for k in range(1, nd):
        whole = pltpu.make_async_remote_copy(
            belows.at[k - 1],
            belows.at[k - 1],
            send_q.at[k - 1],
            recv_q.at[k - 1],
            device_id=peer_of(k, 0, nd, ntr),
            device_id_type=MESH,
        )

        @pl.when(d + k < nd)
        def _():
            whole.wait_recv()
            for col in range(ntr // per):
                below_sum[col] = below_sum[col] + track_row(belows.at[k - 1], col)

        @pl.when(d >= k)
        def _():
            whole.wait_send()

    tops = [below_sum[col] for col in range(ntr // per)]
    extra = tops[0]
    for top in tops[1:]:
        extra = extra + top
    extra = jnp.broadcast_to(extra[1:2], (8, LANES))
    below = jnp.concatenate([top[0:1] for top in tops], axis=1) + joined3(nn(split3(extra), side_of[...]))[0:1]
    below = jnp.broadcast_to(below, (nblock, ntr * groups))
    blocks = jnp.broadcast_to(block_of[...].astype(f32)[0:1], (nblock, ntr * groups))
    spread_below = jnp.where(blocks == iota((nblock, ntr * groups), 0).astype(f32), below, 0.0)
    rows_of[...] = joined3(nn(split3(spread_below), place_of[...]))

    @pl.loop(0, nblock, unroll=8)
    def _(j):
        lanes = pl.ds(pl.multiple_of(j * WIDE, WIDE), WIDE)
        grad[:, lanes] = grad[:, lanes] + jnp.broadcast_to(rows_of[pl.ds(j, 1), :], (depth, WIDE))


T_UNROLL = 4
SPREAD_UNROLL = 32
OUTER_UNROLL = 32
OUT_PARTS = 1
AT_ONCE = 8


def on_device(nd, ntr, slowness_cells, cell_of_group, taper, secant, primary, quadrature, observed):
    depth, traces, angles = primary.shape
    taps = taper.shape[1]
    ncell = slowness_cells.shape[1]
    groups = cell_of_group.shape[0]
    nedge = groups * 8
    total = ntr * groups
    nchunk = depth // AT_ONCE
    vmem = pl.BlockSpec(memory_space=pltpu.VMEM)
    anywhere = pl.BlockSpec(memory_space=pl.ANY)
    near = nd - 1
    dma = pltpu.SemaphoreType.DMA
    V = pltpu.VMEM
    slow = slowness_cells.reshape(depth // 8, 8, ncell // LANES, LANES).transpose(0, 2, 1, 3)
    gradient, image = pl.pallas_call(
        functools.partial(main_kernel, nd, ntr, nchunk),
        out_shape=(
            jax.ShapeDtypeStruct((depth, ncell), f32),
            jax.ShapeDtypeStruct((depth, traces), f32),
        ),
        in_specs=[anywhere] * 7,
        out_specs=(vmem, vmem),
        scratch_shapes=[
            pltpu.SMEM((groups,), jnp.int32),
            V((taps, angles), f32),
            V((1, angles), f32),
            V((depth, traces), f32),
            V(slow.shape, f32),
            V((depth, traces, angles), bf16),
            V((depth, traces, angles), bf16),
            V((3, 8, angles), f32),
            V((depth, LANES), f32),
            V((depth, 24, LANES), f32),
            V((depth, traces), f32),
            V((depth, traces), f32),
        ]
        + [V((depth, nedge), f32)] * 6
        + [
            V((nedge, traces), bf16),
            V((traces, LANES), bf16),
            V((nedge, LANES), bf16),
            V((nedge, LANES), bf16),
            V((depth, LANES), f32),
            V((8 * near, LANES), f32),
            V((2 * depth + 16 * near, LANES), f32),
            V((ntr * groups // LANES, 2, LANES), f32),
            V((1, LANES), f32),
            V((ntr, 1, LANES), f32),
            V((LANES, total), bf16),
            V((depth, groups + traces // 256, 2, 8, angles), f32),
            V((groups + traces // 256, 2, 8, angles), f32),
            V((1, LANES), f32),
            V((ntr, 1, LANES), f32),
            V((4, LANES), f32),
            V((ntr, 4, LANES), f32),
            V((2, LANES), f32),
            V((near, ntr, 2, LANES), f32),
            V((depth, total), bf16),
            V((depth, total), bf16),
            V((depth, total), bf16),
            V((total, WIDE), bf16),
            V((ncell // WIDE, WIDE), f32),
            dma((4,)),
            dma,
            dma((nchunk,)),
            dma((nchunk,)),
        ]
        + [dma] * 10
        + [dma((near,))] * 2,
        compiler_params=pltpu.CompilerParams(
            collective_id=0,
            has_side_effects=True,
            vmem_limit_bytes=VMEM_LIMIT,
        ),
        name="radargram",
    )(
        *[
            pltpu.with_memory_space_constraint(v, pltpu.HBM)
            for v in (slow, cell_of_group, taper.T, secant.reshape(1, angles), primary, quadrature, observed)
        ]
    )
    gradient, image = pl.pallas_call(
        hand_out,
        out_shape=(
            jax.ShapeDtypeStruct((depth, ncell), f32),
            jax.ShapeDtypeStruct((depth, traces), f32),
        ),
        in_specs=[anywhere] * 2,
        out_specs=(anywhere, anywhere),
        scratch_shapes=[dma((OUT_PARTS + 1,))],
        compiler_params=pltpu.CompilerParams(vmem_limit_bytes=1024 * 1024),
        name="hand_out",
    )(gradient, image)
    return image, gradient


def hand_out(grad, image, grad_out, image_out, sems):
    rows = grad.shape[0] // OUT_PARTS
    copies = [pltpu.make_async_copy(image, image_out, sems.at[OUT_PARTS])]
    for i in range(OUT_PARTS):
        part = pl.ds(i * rows, rows)
        copies.append(pltpu.make_async_copy(grad.at[part], grad_out.at[part], sems.at[i]))
    for copy in copies:
        copy.start()
    for copy in copies:
        copy.wait()


VMEM_LIMIT = 40 * 1024 * 1024


def solution(mesh):
    in_specs = (
        P("depth", None),
        P("track"),
        P(),
        P(),
        P("depth", "track", None),
        P("depth", "track", None),
        P("depth", "track"),
    )
    out_specs = (P("depth", "track"), P("depth", None))
    nd = mesh.shape["depth"]
    ntr = mesh.shape["track"]
    return jax.shard_map(
        functools.partial(on_device, nd, ntr), mesh=mesh, in_specs=in_specs, out_specs=out_specs, check_vma=False
    )
```

```python
import functools
import math

import jax
import jax.numpy as jnp
from jax import lax
from jax.experimental import pallas as pl
from jax.experimental.pallas import tpu as pltpu
from jax.sharding import PartitionSpec as P

OMEGA = 0.25
GROUP = 32
LANES = 128
MESH = pl.DeviceIdType.MESH

SIN = (4.442882919178189, -7.308245695274183, 3.6063544029247794, -0.8461128632742358, 0.10982698821149484)
COS = (1.4142134964903517, -6.978850985165349, 5.739461140914948, -1.8835629076104397, 0.310698190958135)

f32 = jnp.float32
bf16 = jnp.bfloat16


def horner(coefs, u):
    value = coefs[-1] * u + coefs[-2]
    for c in coefs[-3::-1]:
        value = value * u + c
    return value


def cos_sin(turns):
    r = turns - jnp.round(turns)
    u = r * r
    s = r * horner(SIN, u)
    c = horner(COS, u)
    return 1.0 - s * s, s * c


def iota(shape, dim):
    return lax.broadcasted_iota(jnp.int32, shape, dim)


def part(x, n):
    return lax.shift_right_logical(x, n.bit_length() - 1)


def inside_part(x, n):
    return x & (n - 1)


def nt(a, b):
    return lax.dot_general(a, b, (((1,), (1,)), ((), ())), preferred_element_type=f32)


def nn(a, b):
    return lax.dot_general(a, b, (((1,), (0,)), ((), ())), preferred_element_type=f32)


def split3(x):
    high = x.astype(bf16).astype(f32)
    rest = x - high
    mid = rest.astype(bf16).astype(f32)
    return jnp.concatenate([high, mid, rest - mid], axis=0).astype(bf16)


def joined3(y):
    n = y.shape[0] // 3
    return y[:n] + y[n : 2 * n] + y[2 * n :]


def one_hot(mask):
    return jnp.where(mask, 1.0, 0.0).astype(bf16)


def peer_of(k, o, nd, nt_):
    d = lax.axis_index("depth")
    t = lax.axis_index("track")
    return (lax.rem(d + k, nd), lax.rem(t + o + nt_, nt_))


def near_copies(nd, nt_, src, tile, into, send, recv):
    return [
        pltpu.make_async_remote_copy(
            src.at[pl.ds(tile, 8)],
            into.at[pl.ds(8 * (k - 1), 8)],
            send,
            recv,
            device_id=peer_of(k, 0, nd, nt_),
            device_id_type=MESH,
        )
        for k in range(1, nd)
    ]


def side_copies(nd, nt_, src, tile, into, send, recv):
    depth = src.shape[0]
    copies = []
    for i, o in enumerate((1, -1)):
        copies.append(
            pltpu.make_async_remote_copy(
                src,
                into.at[pl.ds(i * depth, depth)],
                send,
                recv,
                device_id=peer_of(0, o, nd, nt_),
                device_id_type=MESH,
            )
        )
        for k in range(1, nd):
            copies.append(
                pltpu.make_async_remote_copy(
                    src.at[pl.ds(tile, 8)],
                    into.at[pl.ds(2 * depth + 8 * (2 * (k - 1) + i), 8)],
                    send,
                    recv,
                    device_id=peer_of(k, o, nd, nt_),
                    device_id_type=MESH,
                )
            )
    return copies


def wait_all(into, send, recv, nd, nt_):
    copy = pltpu.make_async_remote_copy(
        into, into, send, recv, device_id=peer_of(1, 0, nd, nt_), device_id_type=MESH
    )
    copy.wait_recv()
    copy.wait_send()


WIDE = 256
PER_STEP = 32


def main_kernel(
    nd,
    ntr,
    nchunk,
    slow_hbm,
    cells_hbm,
    taper_hbm,
    secant_hbm,
    prim_hbm,
    quad_hbm,
    seen_hbm,
    grad,
    focused,
    cells,
    taper,
    secant,
    seen,
    slow,
    prim,
    quad,
    weights,
    line,
    spread,
    fint,
    bint,
    fedge,
    blo,
    bhi,
    fside,
    loside,
    hiside,
    edge_of,
    to_own,
    to_lo,
    to_hi,
    halo_a,
    near_a,
    side_a,
    below_sum,
    sides_mine,
    sides,
    side_of,
    phase,
    rot,
    cells_mine,
    cell_rows,
    mine,
    packets,
    below_mine,
    belows,
    ghigh,
    glow,
    block_of,
    place_of,
    rows_of,
    small_sem,
    slow_sem,
    prim_sem,
    quad_sem,
    send_a,
    recv_a,
    send_as,
    recv_as,
    send_cells,
    recv_cells,
    send_s,
    recv_s,
    send_p,
    recv_p,
    send_q,
    recv_q,
):
    d = lax.axis_index("depth")
    t = lax.axis_index("track")
    depth, traces, angles = prim.shape
    groups = traces // GROUP
    zc = depth // nchunk
    per = LANES // groups

    barrier = pltpu.get_barrier_semaphore()
    slow_copy = pltpu.make_async_copy(slow_hbm, slow, slow_sem)
    small = [
        pltpu.make_async_copy(cells_hbm, cells, small_sem.at[0]),
        pltpu.make_async_copy(taper_hbm, taper, small_sem.at[1]),
        pltpu.make_async_copy(secant_hbm, secant, small_sem.at[2]),
        pltpu.make_async_copy(seen_hbm, seen, small_sem.at[3]),
    ]
    small[0].start()
    slow_copy.start()

    @pl.loop(1, ntr)
    def _(k):
        pl.semaphore_signal(barrier, inc=1, device_id=(d, lax.rem(t + k, ntr)), device_id_type=MESH)

    for k in range(1, nd):
        for o in (-1, 0, 1):
            pl.semaphore_signal(barrier, inc=1, device_id=peer_of(k, o, nd, ntr), device_id_type=MESH)
    for copy in small[1:]:
        copy.start()

    def chunk_copies(i):
        rows = pl.ds(i * zc, zc)
        return (
            pltpu.make_async_copy(prim_hbm.at[rows], prim.at[rows], prim_sem.at[i]),
            pltpu.make_async_copy(quad_hbm.at[rows], quad.at[rows], quad_sem.at[i]),
        )

    mine_lane = iota((depth, LANES), 1)
    zrow = iota((depth, LANES), 0)
    small[0].wait()
    slow_copy.wait()

    @pl.loop(0, nchunk)
    def _(i):
        for copy in chunk_copies(i):
            copy.start()

    own = jnp.zeros((depth, LANES), f32)
    for g in range(groups):
        c = cells[g]
        block = slow[:, lax.div(c, LANES)].reshape(depth, LANES)
        column = jnp.sum(jnp.where(mine_lane == lax.rem(c, LANES), block, 0.0), axis=1, keepdims=True)
        own = jnp.where(mine_lane == g, column, own)
    s = 1
    while s < depth:
        own = own + jnp.where(zrow >= s, pltpu.roll(own, s, 0), 0.0)
        s *= 2
    halo_a[...] = own

    pl.semaphore_wait(barrier, ntr - 1 + 3 * (nd - 1))
    for copy in near_copies(nd, ntr, halo_a, depth - 8, near_a, send_a, recv_a):
        copy.start()
    for copy in side_copies(nd, ntr, halo_a, depth - 8, side_a, send_as, recv_as):
        copy.start()

    lane1 = iota((1, LANES), 1)
    shift = groups * lax.rem(t, per)
    row = jnp.zeros((1, LANES), f32)
    for g in range(groups):
        row = jnp.where(lane1 == shift + g, cells[g].astype(f32), row)
    cells_mine[...] = row
    cell_rows[t] = row

    def to_track(k, src, into, send, recv):
        pltpu.make_async_remote_copy(
            src,
            into.at[t],
            send,
            recv,
            device_id=(d, lax.rem(t + k, ntr)),
            device_id_type=MESH,
        ).start()

    @pl.loop(1, ntr)
    def _(k):
        to_track(k, cells_mine, cell_rows, send_cells, recv_cells)

    def others(ref):
        return ref.at[pl.ds(0, ntr - 1)]

    def track_row(ref, col):
        acc = ref[col * per]
        for j in range(1, per):
            acc = acc + ref[col * per + j]
        return acc

    for copy in small[1:]:
        copy.wait()
    taps = taper[...]
    sec = secant[...] * OMEGA
    row = iota((8, angles), 0)
    nlo = jnp.where(row < 4, 4 - row, 12 - row)
    wlo = jnp.zeros((8, angles), f32)
    whi = jnp.zeros((8, angles), f32)
    for k in range(taper.shape[0]):
        tap = jnp.broadcast_to(taps[k : k + 1, :] * sec, (8, angles))
        wlo = wlo + jnp.where(k < nlo, tap, 0.0)
        whi = whi + jnp.where(k < nlo, 0.0, tap)
    weights[0] = wlo
    weights[1] = whi
    weights[2] = jnp.broadcast_to(jnp.sum(taps, axis=0, keepdims=True) * sec, (8, angles))

    nedge = groups * 8
    e = iota((nedge, traces), 0)
    x = iota((nedge, traces), 1)
    i = inside_part(e, 8)
    at = inside_part(part(e, 8) * GROUP + jnp.where(i < 4, i, i - 8) + traces, traces)
    edge_of[...] = one_hot(at == x)
    to_own[...] = one_hot(part(iota((traces, LANES), 0), GROUP) == iota((traces, LANES), 1))
    eb = iota((nedge, LANES), 0)
    el = iota((nedge, LANES), 1)
    bi = part(eb, 8)
    behind_row = inside_part(eb, 8) < 4
    to_lo[...] = one_hot(jnp.where(bi > 0, bi - 1, jnp.where(behind_row, groups, groups - 1)) == el)
    to_hi[...] = one_hot(jnp.where((bi > 0) | behind_row, bi, groups + 1) == el)
    seen_edge = joined3(nt(split3(seen[...]), edge_of[...]))

    def near_total(into, rowi, up):
        acc = jnp.zeros((1, LANES), f32)
        for k in range(1, nd):
            at = 8 * (k - 1) + rowi
            acc = acc + jnp.where((k <= d) if up else (k > d), into[at : at + 1, :], 0.0)
        return acc

    def side_total(i, rowi, into, up):
        acc = into[i * depth : (i + 1) * depth, :]
        for k in range(1, nd):
            use = (k <= d) if up else (k > d)
            at = 2 * depth + 8 * (2 * (k - 1) + i) + rowi
            acc = acc + jnp.where(use, into[at : at + 1, :], 0.0)
        return acc

    turn = 1.0 / (2.0 * math.pi)
    line[...] = own * turn

    def spread_rows(first, count):
        diagonal = iota((count, LANES), 0) + first == iota((count, LANES), 1)

        @pl.loop(0, depth, unroll=SPREAD_UNROLL)
        def _(z):
            lines = jnp.broadcast_to(line[pl.ds(z, 1), :], (count, LANES))
            spread[z, first : first + count, :] = jnp.broadcast_to(
                jnp.sum(jnp.where(diagonal, lines, 0.0), axis=1, keepdims=True), (count, LANES)
            )

    spread_rows(0, groups)

    sub = iota((8, angles), 0)
    upper = sub < 4
    sub128 = iota((8, LANES), 0)
    lane128 = iota((8, LANES), 1)
    place = inside_part(lane128, 8) == sub128
    half = 256
    own_group = sub == part(iota((8, half), 1), GROUP)

    def splat(z, r):
        return jnp.broadcast_to(spread[z, r : r + 1, :], (8, LANES))

    def widened(v):
        return jnp.concatenate([v] * (angles // LANES), axis=1)

    nhalf = traces // half

    def local_phases(z):
        for h in range(nhalf):
            c, s = cos_sin(weights[2] * widened(spread[z, 8 * h : 8 * h + 8, :]))
            phase[z, groups + h, 0] = c
            phase[z, groups + h, 1] = s
        for b in range(1, groups):
            c, s = cos_sin(weights[0] * widened(splat(z, b - 1)) + weights[1] * widened(splat(z, b)))
            phase[z, b, 0] = c
            phase[z, b, 1] = s

    def edge_rows(ref, z, b):
        behind = ref[z, GROUP * b : GROUP * b + 8, :].astype(f32)
        stop = GROUP * b if b else traces
        before = ref[z, stop - 8 : stop, :].astype(f32)
        return jnp.where(upper, behind, before)

    def edge_sums(pe, qe, c, s):
        g = qe * c - pe * s
        return [jnp.sum(v, axis=1, keepdims=True) for v in (pe * c + qe * s, g * weights[0], g * weights[1])]

    def inside(z):
        for h in range(nhalf):
            c0 = phase[z, groups + h, 0]
            s0 = phase[z, groups + h, 1]
            ca = rot[groups + h, 0]
            sa = rot[groups + h, 1]
            c = c0 * ca - s0 * sa
            s = s0 * ca + c0 * sa
            w = weights[2]
            wc = w * c
            ws = w * s

            def pair(v):
                return [v, v - v.astype(bf16).astype(f32)]

            lhs_p = jnp.concatenate(pair(c) + pair(-ws), axis=0).astype(bf16)
            lhs_q = jnp.concatenate(pair(s) + pair(wc), axis=0).astype(bf16)
            rows = pl.ds(h * half, half)
            out = nt(lhs_p, prim[z, rows, :]) + nt(lhs_q, quad[z, rows, :])
            fsum = jnp.where(own_group, out[0:8] + out[8:16], 0.0)
            bsum = jnp.where(own_group, out[16:24] + out[24:32], 0.0)
            fint[pl.ds(z, 1), rows] = jnp.sum(fsum, axis=0, keepdims=True)
            bint[pl.ds(z, 1), rows] = jnp.sum(bsum, axis=0, keepdims=True)

    def boundary(zs, b, accs):
        here = part(lane128, 8) == b
        ca = rot[b, 0]
        sa = rot[b, 1]
        out = []
        for z, acc in zip(zs, accs):
            p = edge_rows(prim, z, b)
            q = edge_rows(quad, z, b)
            found = edge_sums(p * ca + q * sa, q * ca - p * sa, phase[z, b, 0], phase[z, b, 1])
            out.append([jnp.where(here, v, a) for v, a in zip(found, acc)])
        return out

    def each_depth(zs):
        accs = [[jnp.zeros((8, LANES), f32)] * 3 for _ in zs]
        every = max(1, (groups - 1) // len(zs))
        for b in range(1, groups):
            if (b - 1) % every == 0 and (b - 1) // every < len(zs):
                inside(zs[(b - 1) // every])
            accs = boundary(zs, b, accs)
        for z, acc in zip(zs, accs):
            for a, ref in zip(acc, (fedge, blo, bhi)):
                ref[pl.ds(z, 1), :] = jnp.sum(jnp.where(place, a, 0.0), axis=0, keepdims=True)

    def outer_edge(z):
        before = jnp.where(sub128 < 4, splat(z, groups), splat(z, groups + 3))
        behind = jnp.where(sub128 < 4, splat(z, groups + 2), splat(z, groups + 1))
        c, s = cos_sin(weights[0] * widened(before) + weights[1] * widened(behind))
        found = edge_sums(edge_rows(prim, z, 0), edge_rows(quad, z, 0), c, s)
        for v, ref in zip(found, (fside, loside, hiside)):
            picked = jnp.where(place & (lane128 < 8), v, 0.0)
            ref[pl.ds(z, 1), :] = jnp.sum(picked, axis=0, keepdims=True)

    @pl.loop(0, depth, unroll=T_UNROLL)
    def _(z):
        local_phases(z)

    wait_all(near_a, send_a, recv_a, nd, ntr)
    above = near_total(near_a, 7, True)
    diagonal = iota((groups, LANES), 0) == iota((groups, LANES), 1)
    lines = jnp.where(diagonal, jnp.broadcast_to(above * turn, (groups, LANES)), 0.0)
    above_rows = jnp.broadcast_to(jnp.sum(lines, axis=1, keepdims=True), (groups, LANES))
    for h in range(nhalf):
        c, s = cos_sin(weights[2] * widened(above_rows[8 * h : 8 * h + 8]))
        rot[groups + h, 0] = c
        rot[groups + h, 1] = s
    for b in range(1, groups):
        lo = jnp.broadcast_to(above_rows[b - 1 : b], (8, LANES))
        hi = jnp.broadcast_to(above_rows[b : b + 1], (8, LANES))
        c, s = cos_sin(weights[0] * widened(lo) + weights[1] * widened(hi))
        rot[b, 0] = c
        rot[b, 1] = s

    @pl.loop(0, nchunk)
    def _(i):
        for copy in chunk_copies(i):
            copy.wait()

        each_depth([i * zc + j for j in range(zc)])

    wait_all(side_a, send_as, recv_as, nd, ntr)
    left = jnp.where(t > 0, side_total(0, 7, side_a, True), 0.0) * turn
    right = jnp.where(t < ntr - 1, side_total(1, 7, side_a, True), 0.0) * turn
    centre = (own + above) * turn
    outer = jnp.where(mine_lane == groups, pltpu.roll(left, 1, 1), 0.0)
    outer = jnp.where(mine_lane == groups + 1, pltpu.roll(right, groups + 1, 1), outer)
    outer = jnp.where(mine_lane == groups + 2, pltpu.roll(centre, groups + 2, 1), outer)
    line[...] = jnp.where(mine_lane == groups + 3, pltpu.roll(centre, 4, 1), outer)
    spread_rows(groups, 8)

    @pl.loop(0, depth, unroll=OUTER_UNROLL)
    def _(z):
        outer_edge(z)

    def suffix(v):
        s = 1
        while s < depth:
            v = v + jnp.where(zrow < depth - s, pltpu.roll(v, depth - s, 0), 0.0)
            s *= 2
        return v

    xoff = inside_part(iota((depth, traces), 1), GROUP)
    inner = (xoff >= 4) & (xoff < GROUP - 4)
    term = jnp.where(inner, (fint[...] - seen[...]) * bint[...], 0.0)
    edge = fedge[...] + fside[...]
    resid = edge - seen_edge
    sums = joined3(nn(split3(term), to_own[...]))
    sums = sums + joined3(nn(split3(resid * (blo[...] + loside[...])), to_lo[...]))
    sums = sums + joined3(nn(split3(resid * (bhi[...] + hiside[...])), to_hi[...]))
    sums = jnp.where((t == 0) & (mine_lane == groups), 0.0, sums)
    sums = jnp.where((t == ntr - 1) & (mine_lane == groups + 1), 0.0, sums)
    sums = suffix(sums)

    total_row = jnp.broadcast_to(sums[0:1], (8, LANES))
    below = pltpu.roll(jnp.where(lane128 < groups, total_row, 0.0), shift, 1)
    before = pltpu.roll(jnp.where(lane128 == groups, total_row, 0.0), lax.rem(t + LANES - groups, LANES), 1)
    behind = pltpu.roll(
        jnp.where(lane128 == groups + 1, total_row, 0.0), lax.rem(t + LANES + ntr - groups - 1, LANES), 1
    )
    below_mine[...] = jnp.where(sub128 == 0, below, before + behind)[0:2]

    def above_copy(k, o):
        return pltpu.make_async_remote_copy(
            below_mine,
            belows.at[k - 1, t],
            send_q.at[k - 1],
            recv_q.at[k - 1],
            device_id=(lax.rem(d + nd - k, nd), lax.rem(t + o, ntr)),
            device_id_type=MESH,
        )

    for k in range(nd - 1, 0, -1):

        @pl.when(d >= k)
        def _():
            @pl.loop(0, ntr)
            def _(o):
                above_copy(k, lax.rem(o + ntr // 2, ntr)).start()

    grads = jnp.where(mine_lane < groups, sums, 0.0)
    packet = jnp.zeros((8, LANES), f32)
    for q in range(depth // 8):
        block = grads[8 * q : 8 * q + 8]
        packet = packet + (pltpu.roll(block, groups * q, 1) if q else block)
    packet = packet + pltpu.roll(pltpu.roll(packet, 4, 0), LANES // 2, 1)
    packet = pltpu.roll(packet, shift, 1)[0:4]
    mine[...] = packet
    packets[t] = packet

    @pl.loop(1, ntr)
    def _(k):
        to_track(k, mine, packets, send_p, recv_p)

    before = jnp.sum(jnp.where(mine_lane == groups, sums, 0.0), axis=1, keepdims=True)
    behind = jnp.sum(jnp.where(mine_lane == groups + 1, sums, 0.0), axis=1, keepdims=True)
    row = jnp.where(mine_lane == zrow, before, jnp.where(mine_lane == zrow + depth, behind, 0.0))
    row = jnp.sum(row, axis=0, keepdims=True)
    sides_mine[...] = row
    sides[t] = row

    @pl.loop(1, ntr)
    def _(k):
        to_track(k, sides_mine, sides, send_s, recv_s)

    wait_all(others(cell_rows), send_cells, recv_cells, nd, ntr)
    for col in range(ntr // per):
        lanes = pl.ds(col * LANES, LANES)
        cell = track_row(cell_rows, col)
        block = jnp.floor(cell * (1.0 / WIDE))
        block_of[:, lanes] = jnp.broadcast_to(block, (depth, LANES)).astype(bf16)
        column = jnp.broadcast_to(cell - block * WIDE, (LANES, LANES)).T
        column = jnp.concatenate([column] * (WIDE // LANES), axis=1)
        place_of[lanes, :] = one_hot(iota((LANES, WIDE), 1).astype(f32) == column)

    srow = iota((LANES, ntr * groups), 0)
    scol = iota((LANES, ntr * groups), 1)
    starget = jnp.where(srow < ntr, srow * groups - 1, (srow - ntr) * groups + groups)
    side_of[...] = one_hot((srow < 2 * ntr) & (starget == scol))

    focused[...] = jnp.where(inner, fint[...], joined3(nn(split3(edge), edge_of[...])))
    wait_all(others(packets), send_p, recv_p, nd, ntr)

    wait_all(others(sides), send_s, recv_s, nd, ntr)
    blocks = []
    for j in range(ntr // 8):
        acc = jnp.zeros((8, LANES), f32)
        for i in range(8):
            acc = jnp.where(sub128 == i, jnp.broadcast_to(sides[8 * j + i], (8, LANES)), acc)
        blocks.append(acc)
    turned = jnp.concatenate(blocks, axis=0).T
    turned = jnp.concatenate([turned[0:depth], turned[depth : 2 * depth]], axis=1)
    side_terms = joined3(nn(split3(turned), side_of[0 : 2 * ntr, :]))
    chunk = part(iota((4, LANES), 1), groups)
    for col in range(ntr // per):
        parts = []
        for c in range(per):
            acc = jnp.zeros((4, LANES), f32)
            for j in range(per):
                acc = jnp.where(chunk == (c + j) % per, packets[col * per + j], acc)
            parts.append(acc)
        lanes = pl.ds(col * LANES, LANES)
        nq = depth // 8
        pieces = []
        for q in range(nq):
            for h in range(2):
                c = q + nq * h
                both = jnp.concatenate([parts[c], parts[c]], axis=0)
                pieces.append(pltpu.roll(both, LANES - groups * c, 1) if c else both)
        low_rows = iota((8, LANES), 0) < 4
        g = jnp.concatenate(
            [jnp.where(low_rows, pieces[2 * q], pieces[2 * q + 1]) for q in range(nq)], axis=0
        )
        g = g + side_terms[:, col * LANES : (col + 1) * LANES]
        high = g.astype(bf16)
        ghigh[:, lanes] = high
        glow[:, lanes] = (g - high.astype(f32)).astype(bf16)

    nblock = grad.shape[1] // WIDE

    @pl.loop(0, nblock // PER_STEP)
    def _(step):
        highs = []
        lows = []
        for j in range(PER_STEP):
            mask = block_of[...] == (step * PER_STEP + j).astype(bf16)
            highs.append(jnp.where(mask, ghigh[...], jnp.zeros((), bf16)))
            lows.append(jnp.where(mask, glow[...], jnp.zeros((), bf16)))
        out = nn(jnp.concatenate(highs, axis=0), place_of[...]) + nn(jnp.concatenate(lows, axis=0), place_of[...])
        out = jnp.concatenate([out[depth * j : depth * (j + 1)] for j in range(PER_STEP)], axis=1)
        wide = PER_STEP * WIDE
        grad[:, pl.ds(pl.multiple_of(step * wide, wide), wide)] = out

    below_sum[...] = jnp.zeros(below_sum.shape, f32)
    for k in range(1, nd):
        whole = pltpu.make_async_remote_copy(
            belows.at[k - 1],
            belows.at[k - 1],
            send_q.at[k - 1],
            recv_q.at[k - 1],
            device_id=peer_of(k, 0, nd, ntr),
            device_id_type=MESH,
        )

        @pl.when(d + k < nd)
        def _():
            whole.wait_recv()
            for col in range(ntr // per):
                below_sum[col] = below_sum[col] + track_row(belows.at[k - 1], col)

        @pl.when(d >= k)
        def _():
            whole.wait_send()

    tops = [below_sum[col] for col in range(ntr // per)]
    extra = tops[0]
    for top in tops[1:]:
        extra = extra + top
    extra = jnp.broadcast_to(extra[1:2], (8, LANES))
    below = jnp.concatenate([top[0:1] for top in tops], axis=1) + joined3(nn(split3(extra), side_of[...]))[0:1]
    below = jnp.broadcast_to(below, (nblock, ntr * groups))
    blocks = jnp.broadcast_to(block_of[...].astype(f32)[0:1], (nblock, ntr * groups))
    spread_below = jnp.where(blocks == iota((nblock, ntr * groups), 0).astype(f32), below, 0.0)
    rows_of[...] = joined3(nn(split3(spread_below), place_of[...]))

    @pl.loop(0, nblock, unroll=8)
    def _(j):
        lanes = pl.ds(pl.multiple_of(j * WIDE, WIDE), WIDE)
        grad[:, lanes] = grad[:, lanes] + jnp.broadcast_to(rows_of[pl.ds(j, 1), :], (depth, WIDE))


T_UNROLL = 4
SPREAD_UNROLL = 32
OUTER_UNROLL = 32
OUT_PARTS = 1
AT_ONCE = 8


def on_device(nd, ntr, slowness_cells, cell_of_group, taper, secant, primary, quadrature, observed):
    depth, traces, angles = primary.shape
    taps = taper.shape[1]
    ncell = slowness_cells.shape[1]
    groups = cell_of_group.shape[0]
    nedge = groups * 8
    total = ntr * groups
    nchunk = depth // AT_ONCE
    vmem = pl.BlockSpec(memory_space=pltpu.VMEM)
    anywhere = pl.BlockSpec(memory_space=pl.ANY)
    near = nd - 1
    dma = pltpu.SemaphoreType.DMA
    V = pltpu.VMEM
    slow = slowness_cells.reshape(depth // 8, 8, ncell // LANES, LANES).transpose(0, 2, 1, 3)
    gradient, image = pl.pallas_call(
        functools.partial(main_kernel, nd, ntr, nchunk),
        out_shape=(
            jax.ShapeDtypeStruct((depth, ncell), f32),
            jax.ShapeDtypeStruct((depth, traces), f32),
        ),
        in_specs=[anywhere] * 7,
        out_specs=(vmem, vmem),
        scratch_shapes=[
            pltpu.SMEM((groups,), jnp.int32),
            V((taps, angles), f32),
            V((1, angles), f32),
            V((depth, traces), f32),
            V(slow.shape, f32),
            V((depth, traces, angles), bf16),
            V((depth, traces, angles), bf16),
            V((3, 8, angles), f32),
            V((depth, LANES), f32),
            V((depth, 24, LANES), f32),
            V((depth, traces), f32),
            V((depth, traces), f32),
        ]
        + [V((depth, nedge), f32)] * 6
        + [
            V((nedge, traces), bf16),
            V((traces, LANES), bf16),
            V((nedge, LANES), bf16),
            V((nedge, LANES), bf16),
            V((depth, LANES), f32),
            V((8 * near, LANES), f32),
            V((2 * depth + 16 * near, LANES), f32),
            V((ntr * groups // LANES, 2, LANES), f32),
            V((1, LANES), f32),
            V((ntr, 1, LANES), f32),
            V((LANES, total), bf16),
            V((depth, groups + traces // 256, 2, 8, angles), f32),
            V((groups + traces // 256, 2, 8, angles), f32),
            V((1, LANES), f32),
            V((ntr, 1, LANES), f32),
            V((4, LANES), f32),
            V((ntr, 4, LANES), f32),
            V((2, LANES), f32),
            V((near, ntr, 2, LANES), f32),
            V((depth, total), bf16),
            V((depth, total), bf16),
            V((depth, total), bf16),
            V((total, WIDE), bf16),
            V((ncell // WIDE, WIDE), f32),
            dma((4,)),
            dma,
            dma((nchunk,)),
            dma((nchunk,)),
        ]
        + [dma] * 10
        + [dma((near,))] * 2,
        compiler_params=pltpu.CompilerParams(
            collective_id=0,
            has_side_effects=True,
            vmem_limit_bytes=VMEM_LIMIT,
        ),
        name="radargram",
    )(
        *[
            pltpu.with_memory_space_constraint(v, pltpu.HBM)
            for v in (slow, cell_of_group, taper.T, secant.reshape(1, angles), primary, quadrature, observed)
        ]
    )
    gradient, image = pl.pallas_call(
        hand_out,
        out_shape=(
            jax.ShapeDtypeStruct((depth, ncell), f32),
            jax.ShapeDtypeStruct((depth, traces), f32),
        ),
        in_specs=[anywhere] * 2,
        out_specs=(anywhere, anywhere),
        scratch_shapes=[dma((OUT_PARTS + 1,))],
        compiler_params=pltpu.CompilerParams(vmem_limit_bytes=1024 * 1024),
        name="hand_out",
    )(gradient, image)
    return image, gradient


def hand_out(grad, image, grad_out, image_out, sems):
    rows = grad.shape[0] // OUT_PARTS
    copies = [pltpu.make_async_copy(image, image_out, sems.at[OUT_PARTS])]
    for i in range(OUT_PARTS):
        part = pl.ds(i * rows, rows)
        copies.append(pltpu.make_async_copy(grad.at[part], grad_out.at[part], sems.at[i]))
    for copy in copies:
        copy.start()
    for copy in copies:
        copy.wait()


VMEM_LIMIT = 40 * 1024 * 1024


def solution(mesh):
    in_specs = (
        P("depth", None),
        P("track"),
        P(),
        P(),
        P("depth", "track", None),
        P("depth", "track", None),
        P("depth", "track"),
    )
    out_specs = (P("depth", "track"), P("depth", None))
    nd = mesh.shape["depth"]
    ntr = mesh.shape["track"]
    return jax.shard_map(
        functools.partial(on_device, nd, ntr), mesh=mesh, in_specs=in_specs, out_specs=out_specs, check_vma=False
    )
```
